512 devices in a mesh: tm: 128 (over x, z, core), space: 4 (over y).
Axes of the slice: x: 4, y: 4, z: 16, core: 2. Of those that a mesh axis runs over, the one named last changes fastest.
Arguments:
- forcing: bfloat16 [2048, 256, 256], P('tm', 'space'), may hold values from -0.59765625 to 0.59765625
- starting_heat: bfloat16 [256, 256], P('space'), may hold values from -3 to 3, as said below
Outputs:
- heat_history: float32 [2048, 256, 256], P('tm', 'space')
- history: float32 [2, 512], P(None, 'tm')
- change: float32 [2, 512], P(None, 'tm')
The draws below stay inside these ranges and needn't reach their ends.
Inputs may be any that keep to these rules, and one draw needn't show every extreme that they name: starting_heat is a combination of the 64 sine modes with both indices from 1 to 8, scaled so that its largest magnitude is 3.
All inputs are finite; a program needn't handle non-finite values.
Results may differ from the reference program's by a relative error of at most 0.0016.
Values may be sent and summed in bfloat16 or wider, within the bound.
No kernel may reach another device: no remote copies, remote signals or barrier semaphores. Data moves between devices by JAX's collectives and lax.ppermute only.
A program may use at most 64 MiB of HBM per device.

```python
import math
import jax
import jax.numpy as jnp
from jax import lax

GRID = 256
FINE_FACTOR = 4
COARSE_FACTOR = 4
ITERS = 2
NT = 2048
C_POINTS = 512
TOP_POINTS = 128


def draw_starting_heat(key, part):
    mode_index = jnp.arange(1, 9, dtype=jnp.int32)
    cell_index = jnp.arange(1, GRID + 1, dtype=jnp.int32)
    product = mode_index[:, None] * cell_index[None, :] % (2 * (GRID + 1))
    sine_rows = jnp.sin(jnp.pi * product.astype(jnp.float32) / (GRID + 1))
    weights = jax.random.normal(key, (8, 8), jnp.float32)
    inner = jnp.dot(weights, sine_rows, precision=lax.Precision.HIGHEST)
    summed = jnp.dot(sine_rows.T, inner, precision=lax.Precision.HIGHEST)
    scaled = 3.0 * summed / jnp.max(jnp.abs(summed))
    return scaled.astype(jnp.bfloat16)


def block_scale(rng, dims, cuts, low, top_value):
    gain = 1.0
    for axis_at, parts in cuts:
        draws = jax.random.uniform(jax.random.fold_in(jax.random.fold_in(rng, 6), axis_at), (parts,), jnp.float32, low / len(cuts), top_value / len(cuts))
        gain = gain * jnp.repeat(jnp.exp(draws), dims[axis_at] // parts).reshape((-1,) + (1,) * (len(dims) - 1 - axis_at))
    return gain


def bell_draw(stream_key, extent, spread, reach, shards=(), kind=jnp.bfloat16):
    level = block_scale(stream_key, extent, shards, -0.22, 0.18) if shards else 1.0
    result = jax.random.normal(stream_key, extent, jnp.float32) * spread * level
    return jnp.minimum(jnp.maximum(result, -reach), reach).astype(kind)


def setup_inputs(seed: int = 0) -> dict:
    keys = jax.random.split(jax.random.key(seed), 3)
    forcing = bell_draw(keys[0], (NT, GRID, GRID), 0.1, 0.59765625, ((0, 128), (1, 4)))
    starting_heat = draw_starting_heat(jax.random.fold_in(keys[2], 71), 0)
    return dict(forcing=forcing, starting_heat=starting_heat)


DURATION = 0.004

def sine_table(sample_locations, number_type):
    numbers = jnp.arange(1, sample_locations + 1, dtype=jnp.int32)
    product = numbers[:, None] * numbers[None, :] % (2 * (sample_locations + 1))
    angles = jnp.pi * product.astype(jnp.float32) / (sample_locations + 1)
    return (math.sqrt(2.0 / (sample_locations + 1)) * jnp.sin(angles)).astype(number_type)

def eigenvalues(sample_locations, first_mode, mode_count):
    numbers = (first_mode + jnp.arange(mode_count, dtype=jnp.int32) + 1).astype(jnp.float32)
    halves = jnp.sin(jnp.pi * numbers / (2 * (sample_locations + 1)))
    return 4.0 * (sample_locations + 1) ** 2 * halves * halves

def smoothing_pass(starts, sources, factor):
    current = starts
    visited = []
    for column in range(sources.shape[1] - 1):
        current = factor * current + sources[:, column]
        visited.append(current)
    return visited

def forward_block(field_block, table_half):
    halved = jnp.dot(field_block.reshape(-1, GRID), table_half, preferred_element_type=jnp.float32)
    halved = lax.optimization_barrier(halved.astype(jnp.bfloat16).reshape(field_block.shape))
    return jnp.einsum('xi,tiy->txy', table_half.astype(jnp.float32), halved.astype(jnp.float32), precision=lax.Precision.HIGHEST)

def reference(forcing, starting_heat):
    table_half = sine_table(GRID, jnp.bfloat16)
    table_full = sine_table(GRID, jnp.float32)
    decay_rates = eigenvalues(GRID, 0, GRID)[:, None] + eigenvalues(GRID, 0, GRID)[None, :]
    increment_duration = DURATION / NT
    per_increment_factor = 1.0 / (1.0 + increment_duration * decay_rates)
    mid_gain = 1.0 / (1.0 + FINE_FACTOR * increment_duration * decay_rates)
    top_gain = 1.0 / (1.0 + FINE_FACTOR * COARSE_FACTOR * increment_duration * decay_rates)
    start_field = forward_block(starting_heat[None], table_half)[0]

    def source_block(field_block):
        return per_increment_factor * forward_block(field_block, table_half)
    grouped = forcing.reshape(C_POINTS, FINE_FACTOR, GRID, GRID)
    sources = lax.map(source_block, grouped)
    values = jnp.zeros((C_POINTS, GRID, GRID), jnp.float32)
    history_rows = []
    change_rows = []
    for iteration in range(ITERS):
        begins = jnp.concatenate([start_field[None], values[:-1]], 0)
        ends_one = smoothing_pass(begins, sources, per_increment_factor)[-1]
        relaxed = per_increment_factor * ends_one + sources[:, -1]
        ends_two = smoothing_pass(jnp.concatenate([start_field[None], relaxed[:-1]], 0), sources, per_increment_factor)[-1]
        residual = sources[:, -1] + per_increment_factor * ends_two - relaxed
        history_rows.append(jnp.sqrt(lax.optimization_barrier(jnp.sum(residual * residual, axis=(1, 2))) / (GRID * GRID)))
        coarse_rhs = residual.reshape(TOP_POINTS, COARSE_FACTOR, GRID, GRID)
        running = coarse_rhs[:, 0]
        for column in range(1, COARSE_FACTOR):
            running = mid_gain * running + coarse_rhs[:, column]

        def advance(carried, source):
            updated = top_gain * carried + source
            return (updated, updated)
        unused, coarse_values = lax.scan(advance, jnp.zeros((GRID, GRID), jnp.float32), running)
        begins = jnp.concatenate([jnp.zeros((1, GRID, GRID), jnp.float32), coarse_values[:-1]], 0)
        pieces = smoothing_pass(begins, coarse_rhs, mid_gain)
        correction = jnp.stack(pieces + [coarse_values], axis=1).reshape(C_POINTS, GRID, GRID)
        values = relaxed + correction
        corr_sq = lax.optimization_barrier(jnp.sum(correction * correction, axis=(1, 2)))
        value_sq = lax.optimization_barrier(jnp.sum(values * values, axis=(1, 2)))
        change_rows.append(jnp.sqrt(corr_sq / value_sq))
    starts = jnp.concatenate([start_field[None], values[:-1]], 0)

    def finish(items):
        begin_value, block_sources, end_value = items
        inside = smoothing_pass(begin_value[None], block_sources[None], per_increment_factor)
        spectral_path = jnp.concatenate([jnp.stack(inside, axis=1)[0], end_value[None]], 0)
        rows_back = jnp.einsum('xi,tiy->txy', table_full, spectral_path, precision=lax.Precision.HIGHEST)
        rows_back = lax.optimization_barrier(rows_back.astype(jnp.bfloat16))
        return jnp.einsum('txi,iy->txy', rows_back.astype(jnp.float32), table_half.astype(jnp.float32), precision=lax.Precision.HIGHEST)
    heat_history = lax.map(finish, (starts, sources, values)).reshape(NT, GRID, GRID)
    return (heat_history, jnp.stack(history_rows), jnp.stack(change_rows))
```

```python
import functools
import math

import jax
import jax.numpy as jnp
import numpy as np
from jax import lax
from jax.experimental import pallas as pl
from jax.experimental.pallas import tpu as pltpu
from jax.sharding import Mesh
from jax.sharding import PartitionSpec as P

FINE_FACTOR = 4
COARSE_FACTOR = 4
DURATION = 0.004
GRID = 256
NT = 2048
SLAB = 64
MODES = 32
STEPS = 16
PAIRS = STEPS // 2
TOPS = 2
CPOINTS = TOPS * COARSE_FACTOR
BLOCKS = 64
F32, BF16 = jnp.float32, jnp.bfloat16


def sine_table():
    numbers = np.arange(1, GRID + 1)
    product = numbers[:, None] * numbers[None, :] % (2 * (GRID + 1))
    angles = np.float32(np.pi) * product.astype(np.float32) / np.float32(GRID + 1)
    sines = np.sin(angles.astype(np.float64)).astype(np.float32)
    return np.float32(math.sqrt(2.0 / (GRID + 1))) * sines


def eigenvalues():
    halves = np.sin(np.pi * np.arange(1, GRID + 1) / (2 * (GRID + 1)))
    return (4.0 * (GRID + 1) ** 2 * halves * halves).astype(np.float32)


def constants():
    full = sine_table()
    half = np.asarray(jnp.asarray(full).astype(BF16)) if False else full.astype(jnp.bfloat16)
    high = full.astype(jnp.bfloat16)
    low = (full - high.astype(np.float32)).astype(jnp.bfloat16)
    packed = half.reshape(8, 2, 16, GRID).transpose(0, 2, 1, 3).reshape(128, 2 * GRID)
    inward = np.zeros((4, 2, SLAB, 2, GRID), jnp.bfloat16)
    out_high = np.zeros((2, GRID, 4, 2, SLAB), jnp.bfloat16)
    out_low = np.zeros((2, GRID, 4, 2, SLAB), jnp.bfloat16)
    for k in range(2):
        inward[:, k, :, k, :] = half.reshape(4, SLAB, GRID)
        out_high[k, :, :, k, :] = high.reshape(GRID, 4, SLAB)
        out_low[k, :, :, k, :] = low.reshape(GRID, 4, SLAB)
    wide = 2 * GRID
    return (
        half,
        packed,
        inward.reshape(wide, wide),
        out_high.reshape(wide, wide),
        out_low.reshape(wide, wide),
    )


def mul(a, b):
    return None if a is None or b is None else a * b


def add(a, b):
    return b if a is None else a if b is None else a + b


def sub(a, b):
    if b is None:
        return a
    return -b if a is None else a - b


def gains(rates):
    step = DURATION / NT
    gain = 1.0 / (1.0 + step * rates)
    mid = 1.0 / (1.0 + FINE_FACTOR * step * rates)
    top = 1.0 / (1.0 + FINE_FACTOR * COARSE_FACTOR * step * rates)
    square = gain * gain
    return gain, square * square, mid, top


def coarse_pass(entering, residual, mid, top):
    corrections = []
    for first in range(0, len(residual), COARSE_FACTOR):
        rows = residual[first : first + COARSE_FACTOR]
        running, inside = rows[0], entering
        for column in range(1, COARSE_FACTOR):
            inside = add(mul(mid, inside), rows[column - 1])
            corrections.append(inside)
            running = add(mul(mid, running), rows[column])
        entering = add(mul(top, entering), running)
        corrections.append(entering)
    return corrections, entering


def two_iterations(state, first_value, sums, quad, mid, top):
    relaxed_in, error_in, relaxed2_in, error2_in = state
    count = len(sums)
    relaxed = [add(mul(quad, first_value), sums[0])] + list(sums[1:])
    residual = [mul(quad, sub(relaxed_in, first_value))]
    residual += [mul(quad, relaxed[c - 1]) for c in range(1, count)]
    fix, error_out = coarse_pass(error_in, residual, mid, top)
    values = [add(r, p) for r, p in zip(relaxed, fix)]
    before = [add(relaxed_in, error_in)] + values[:-1]
    relaxed2 = [add(mul(quad, v), s) for v, s in zip(before, sums)]
    residual2 = [
        mul(quad, sub(r, v)) for r, v in zip([relaxed2_in] + relaxed2[:-1], before)
    ]
    fix2, error2_out = coarse_pass(error2_in, residual2, mid, top)
    values2 = [add(r, p) for r, p in zip(relaxed2, fix2)]
    leaving = (relaxed[-1], error_out, relaxed2[-1], error2_out)
    return leaving, (residual, fix, values), (residual2, fix2, values2)


def at_start():
    return jnp.logical_and(lax.axis_index("tm_0") == 0, lax.axis_index("tm_1") == 0)


def mode_slab():
    return lax.axis_index("tm_2") * 4 + lax.axis_index("space")


def slab_rates(column_ref, row_ref):
    first = pl.multiple_of(mode_slab() * MODES, MODES)
    columns = column_ref[pl.ds(first, MODES), :]
    return jnp.concatenate([columns, columns], axis=1) + row_ref[...]


def dot(a, b, dims):
    return lax.dot_general(a, b, (dims, ((), ())), preferred_element_type=F32)


def half_kernel(forcing_ref, start_ref, table_ref, packed_ref, out_ref):
    table = table_ref[...]
    for pair in range(PAIRS):
        rows = forcing_ref[pl.ds(128 * pair, 128), :]
        halved = dot(table, rows, ((1,), (1,))).astype(BF16)
        for slab in range(8):
            out_ref[slab, pl.ds(MODES * pair, MODES), :] = halved[MODES * slab : MODES * (slab + 1)]
    start = start_ref[...]
    nothing = jnp.zeros_like(start)
    wide = jnp.concatenate(
        [
            jnp.concatenate([start, nothing], axis=1),
            jnp.concatenate([nothing, start], axis=1),
        ],
        axis=0,
    )
    halved = dot(packed_ref[...], wide, ((1,), (1,))).astype(BF16)
    for slab in range(8):
        out_ref[slab, pl.ds(MODES * PAIRS, 16), :] = halved[16 * slab : 16 * (slab + 1)]


def source_kernel(
    turned_ref, table_ref, column_ref, row_ref, sources_ref, sums_ref, start_ref, local_ref
):
    gain, quad, mid, top = gains(slab_rates(column_ref, row_ref))
    for core in range(2):
        rows = MODES * PAIRS + (16 if core == 0 else 0)
        lhs = jnp.concatenate(
            [turned_ref[4 * core + y, pl.ds(0, rows), :] for y in range(4)], axis=1
        )
        spectra = dot(lhs, table_ref[...], ((1,), (0,)))
        for pair in range(PAIRS):
            for parity in range(2):
                part = spectra[
                    MODES * pair : MODES * (pair + 1), GRID * parity : GRID * (parity + 1)
                ]
                sources_ref[STEPS * core + 2 * pair + parity] = gain * part
        if core == 0:
            last = spectra[MODES * PAIRS :]
            start_ref[...] = jnp.concatenate([last[:, :GRID], last[:, GRID:]], axis=0)
    sums = []
    for point in range(CPOINTS):
        total = sources_ref[FINE_FACTOR * point]
        for step in range(1, FINE_FACTOR):
            total = gain * total + sources_ref[FINE_FACTOR * point + step]
        sums_ref[point] = total
        sums.append(total)
    begin = jnp.where(at_start(), start_ref[...], 0.0)
    leaving, _, _ = two_iterations((begin, None, begin, None), begin, sums, quad, mid, top)
    for index, array in enumerate(leaving):
        for side in range(2):
            local_ref[pl.ds(4 * side + index, MODES, stride=8), :] = array[
                :, 128 * side : 128 * (side + 1)
            ]


def scan_kernel(local_ref, column_ref, row_ref, state_ref):
    chip = lax.axis_index("tm_0") * 16 + lax.axis_index("tm_1")
    column = column_ref[pl.ds(mode_slab() * MODES + chip // 2, 1), :]
    row = jnp.where(chip % 2 == 0, row_ref[:, :128], row_ref[:, 128:])
    _, quad, mid, top = gains(column + row)
    units = []
    for index in range(3):
        state = [None] * 4
        state[index] = jnp.ones_like(top)
        units.append(two_iterations(state, None, [None] * CPOINTS, quad, mid, top)[0])
    power = top
    for _ in range(1, TOPS):
        power = power * top
    relaxed = error = relaxed2 = error2 = jnp.zeros_like(top)
    for block in range(BLOCKS):
        for index, array in enumerate((relaxed, error, relaxed2, error2)):
            state_ref[pl.ds(4 * block + index, 1), :] = array
        local = [local_ref[pl.ds(4 * block + index, 1), :] for index in range(4)]
        error2 = power * error2 + (
            local[3] + units[0][3] * relaxed + units[1][3] * error + units[2][3] * relaxed2
        )
        relaxed2 = units[1][2] * error + (local[2] + units[0][2] * relaxed)
        error = power * error + (local[1] + units[0][1] * relaxed)
        relaxed = local[0]


def path_kernel(
    state_ref, sources_ref, sums_ref, start_ref, high_ref, low_ref, column_ref, row_ref, out_ref
):
    gain, quad, mid, top = gains(slab_rates(column_ref, row_ref))
    state = [
        jnp.concatenate(
            [state_ref[pl.ds(4 * side + index, MODES, stride=8), :] for side in range(2)], axis=1
        )
        for index in range(4)
    ]
    first = at_start()
    start = start_ref[...]
    begin = jnp.where(first, start, 0.0)
    state[0] = jnp.where(first, start, state[0])
    state[2] = jnp.where(first, start, state[2])
    sums = [sums_ref[point] for point in range(CPOINTS)]
    _, one, two = two_iterations(state, begin, sums, quad, mid, top)

    def square_sum(array):
        column = jnp.sum(array * array, axis=0, keepdims=True)
        return jnp.sum(column[:, :128] + column[:, 128:], axis=1, keepdims=True)

    lane = lax.broadcasted_iota(jnp.int32, (1, 128), 1)
    for core in range(2):
        lines = []
        for kind in range(3):
            for which in (one, two):
                line = jnp.zeros((1, 128), F32)
                for point in range(4):
                    total = square_sum(which[kind][4 * core + point])
                    line = jnp.where(lane % 4 == point, total, line)
                lines.append(line)
        lines = jnp.concatenate(lines + [jnp.zeros((10, 128), F32)], axis=0)
        upper = lines.astype(BF16).astype(F32)
        rest = lines - upper
        middle = rest.astype(BF16).astype(F32)
        group = lax.broadcasted_iota(jnp.int32, (16, 128), 1) // 4
        packed = jnp.where(
            group == 0,
            upper,
            jnp.where(group == 1, middle, jnp.where(group == 2, rest - middle, 0.0)),
        ).astype(BF16)
        for y in range(4):
            out_ref[4 * core + y, pl.ds(MODES * PAIRS, 16), :] = packed

    before = [state[2] + state[3]] + two[2][:-1]
    for core in range(2):
        rows = []
        for point in range(4 * core, 4 * core + 4):
            current, visited = before[point], []
            for step in range(FINE_FACTOR - 1):
                current = gain * current + sources_ref[FINE_FACTOR * point + step]
                visited.append(current)
            visited.append(two[2][point])
            rows.append(jnp.concatenate(visited[:2], axis=1))
            rows.append(jnp.concatenate(visited[2:], axis=1))
        path = jnp.concatenate(rows, axis=0)
        high = path.astype(BF16)
        low = (path - high.astype(F32)).astype(BF16)
        turned = dot(high, high_ref[...], ((1,), (0,)))
        turned += dot(high, low_ref[...], ((1,), (0,)))
        turned += dot(low, high_ref[...], ((1,), (0,)))
        turned = turned.astype(BF16)
        for y in range(4):
            out_ref[4 * core + y, pl.ds(0, MODES * PAIRS), :] = turned[:, 128 * y : 128 * (y + 1)]


def heat_kernel(rows_ref, table_ref, heat_ref, history_ref, change_ref):
    table = table_ref[...]
    for pair in range(PAIRS):
        lhs = jnp.concatenate(
            [rows_ref[slab, pl.ds(MODES * pair, MODES), :] for slab in range(8)], axis=0
        )
        heat_ref[pl.ds(128 * pair, 128), :] = dot(lhs, table, ((0,), (0,)))
    total = jnp.zeros((16, 128), F32)
    for slab in range(8):
        total += rows_ref[slab, pl.ds(MODES * PAIRS, 16), :].astype(F32)
    total = total[:, 0:4] + total[:, 4:8] + total[:, 8:12]
    history_ref[...] = jnp.sqrt(total[0:2] / (GRID * GRID))
    change_ref[...] = jnp.sqrt(total[2:4] / total[4:6])


def call(kernel, outs, name):
    single = not isinstance(outs, (list, tuple))
    return pl.pallas_call(
        kernel,
        out_shape=outs if single else tuple(outs),
        compiler_params=pltpu.CompilerParams(vmem_limit_bytes=40 * 1024 * 1024),
        name=name,
    )


def per_device(forcing, starting_heat):
    half, packed, inward, out_high, out_low = (jnp.asarray(c) for c in constants())
    mu = eigenvalues()
    columns = jnp.asarray(np.ascontiguousarray(np.broadcast_to(mu[:, None], (GRID, 128))))
    row = jnp.asarray(mu[None, :])
    shape = jax.ShapeDtypeStruct
    extent = MODES * PAIRS + 16
    ring = ("tm_2", "space")
    plane = ("tm_0", "tm_1")

    halved = call(half_kernel, shape((8, extent, 128), BF16), "half")(
        forcing.reshape(STEPS * SLAB, GRID), starting_heat, half, packed
    )
    turned = lax.all_to_all(halved, ring, 0, 0, tiled=True)
    sources, sums, start, local = call(
        source_kernel,
        [
            shape((2 * STEPS, MODES, GRID), F32),
            shape((CPOINTS, MODES, GRID), F32),
            shape((MODES, GRID), F32),
            shape((4 * BLOCKS, 128), F32),
        ],
        "source",
    )(turned, inward, columns, row)
    gathered = lax.all_to_all(local.reshape(BLOCKS, 4, 128), plane, 0, 0, tiled=True)
    states = call(scan_kernel, shape((4 * BLOCKS, 128), F32), "scan")(
        gathered.reshape(4 * BLOCKS, 128), columns, row
    )
    state = lax.all_to_all(states.reshape(BLOCKS, 4, 128), plane, 0, 0, tiled=True)
    rows = call(path_kernel, shape((8, extent, 128), BF16), "path")(
        state.reshape(4 * BLOCKS, 128), sources, sums, start, out_high, out_low, columns, row
    )
    returned = lax.all_to_all(rows, ring, 0, 0, tiled=True)
    heat, history, change = call(
        heat_kernel,
        [shape((STEPS * SLAB, GRID), F32), shape((2, 4), F32), shape((2, 4), F32)],
        "heat",
    )(returned, half)
    return heat.reshape(STEPS, SLAB, GRID), history, change


def solution(mesh):
    torus = Mesh(
        mesh.devices.reshape(4, 16, 2, mesh.shape["space"]), ("tm_0", "tm_1", "tm_2", "space")
    )
    tm = ("tm_0", "tm_1", "tm_2")
    in_specs = (P(tm, "space", None), P("space", None))
    out_specs = (P(tm, "space", None), P(None, tm), P(None, tm))
    return jax.shard_map(
        per_device, mesh=torus, in_specs=in_specs, out_specs=out_specs, check_vma=False
    )
```

```python
import functools
import math

import jax
import jax.numpy as jnp
import numpy as np
from jax import lax
from jax.experimental import pallas as pl
from jax.experimental.pallas import tpu as pltpu
from jax.sharding import Mesh
from jax.sharding import PartitionSpec as P

FINE_FACTOR = 4
COARSE_FACTOR = 4
DURATION = 0.004
GRID = 256
NT = 2048
SLAB = 64
MODES = 32
STEPS = 16
PAIRS = STEPS // 2
TOPS = 2
CPOINTS = TOPS * COARSE_FACTOR
BLOCKS = 64
F32, BF16 = jnp.float32, jnp.bfloat16


def sine_table():
    numbers = np.arange(1, GRID + 1)
    product = numbers[:, None] * numbers[None, :] % (2 * (GRID + 1))
    angles = np.float32(np.pi) * product.astype(np.float32) / np.float32(GRID + 1)
    sines = np.sin(angles.astype(np.float64)).astype(np.float32)
    return np.float32(math.sqrt(2.0 / (GRID + 1))) * sines


def eigenvalues():
    halves = np.sin(np.pi * np.arange(1, GRID + 1) / (2 * (GRID + 1)))
    return (4.0 * (GRID + 1) ** 2 * halves * halves).astype(np.float32)


def constants():
    full = sine_table()
    half = full.astype(jnp.bfloat16)
    high = full.astype(jnp.bfloat16)
    low = (full - high.astype(np.float32)).astype(jnp.bfloat16)
    inward = np.zeros((4, 2, SLAB, 2, GRID), jnp.bfloat16)
    out_high = np.zeros((2, GRID, 4, 2, SLAB), jnp.bfloat16)
    out_low = np.zeros((2, GRID, 4, 2, SLAB), jnp.bfloat16)
    for k in range(2):
        inward[:, k, :, k, :] = half.reshape(4, SLAB, GRID)
        out_high[k, :, :, k, :] = high.reshape(GRID, 4, SLAB)
        out_low[k, :, :, k, :] = low.reshape(GRID, 4, SLAB)
    wide = 2 * GRID
    return (
        half,
        inward.reshape(wide, wide),
        out_high.reshape(wide, wide),
        out_low.reshape(wide, wide),
    )


def mul(a, b):
    return None if a is None or b is None else a * b


def add(a, b):
    return b if a is None else a if b is None else a + b


def sub(a, b):
    if b is None:
        return a
    return -b if a is None else a - b


def gains(rates):
    step = DURATION / NT
    gain = 1.0 / (1.0 + step * rates)
    mid = 1.0 / (1.0 + FINE_FACTOR * step * rates)
    top = 1.0 / (1.0 + FINE_FACTOR * COARSE_FACTOR * step * rates)
    square = gain * gain
    return gain, square * square, mid, top


def coarse_pass(entering, residual, mid, top):
    corrections = []
    for first in range(0, len(residual), COARSE_FACTOR):
        rows = residual[first : first + COARSE_FACTOR]
        running, inside = rows[0], entering
        for column in range(1, COARSE_FACTOR):
            inside = add(mul(mid, inside), rows[column - 1])
            corrections.append(inside)
            running = add(mul(mid, running), rows[column])
        entering = add(mul(top, entering), running)
        corrections.append(entering)
    return corrections, entering


def two_iterations(state, first_value, sums, quad, mid, top):
    relaxed_in, error_in, relaxed2_in, error2_in = state
    count = len(sums)
    relaxed = [add(mul(quad, first_value), sums[0])] + list(sums[1:])
    residual = [mul(quad, sub(relaxed_in, first_value))]
    residual += [mul(quad, relaxed[c - 1]) for c in range(1, count)]
    fix, error_out = coarse_pass(error_in, residual, mid, top)
    values = [add(r, p) for r, p in zip(relaxed, fix)]
    before = [add(relaxed_in, error_in)] + values[:-1]
    relaxed2 = [add(mul(quad, v), s) for v, s in zip(before, sums)]
    residual2 = [
        mul(quad, sub(r, v)) for r, v in zip([relaxed2_in] + relaxed2[:-1], before)
    ]
    fix2, error2_out = coarse_pass(error2_in, residual2, mid, top)
    values2 = [add(r, p) for r, p in zip(relaxed2, fix2)]
    leaving = (relaxed[-1], error_out, relaxed2[-1], error2_out)
    return leaving, (residual, fix, values), (residual2, fix2, values2)


def at_start():
    return jnp.logical_and(lax.axis_index("tm_0") == 0, lax.axis_index("tm_1") == 0)


def mode_slab():
    return lax.axis_index("tm_2") * 4 + lax.axis_index("space")


def slab_rates(column_ref, row_ref):
    first = pl.multiple_of(mode_slab() * MODES, MODES)
    columns = column_ref[pl.ds(first, MODES), :]
    return jnp.concatenate([columns, columns], axis=1) + row_ref[...]


def dot(a, b, dims):
    return lax.dot_general(a, b, (dims, ((), ())), preferred_element_type=F32)


def half_kernel(
    forcing_hbm, start_hbm, table_hbm, out_ref, forcing_ref, start_ref, table_ref, arrived
):
    copies = [
        pltpu.make_async_copy(table_hbm, table_ref, arrived.at[0]),
        pltpu.make_async_copy(start_hbm, start_ref, arrived.at[1]),
    ]
    parts = 4
    rows = STEPS * SLAB // parts
    for part in range(parts):
        span = pl.ds(part * rows, rows)
        copies.append(
            pltpu.make_async_copy(
                forcing_hbm.at[span, :], forcing_ref.at[span, :], arrived.at[2 + part]
            )
        )
    for copy in copies:
        copy.start()
    copies[0].wait()
    copies[1].wait()
    table = table_ref[...]
    start = start_ref[...]
    nothing = jnp.zeros_like(start)
    wide = jnp.concatenate(
        [
            jnp.concatenate([start, nothing], axis=1),
            jnp.concatenate([nothing, start], axis=1),
        ],
        axis=0,
    )
    packed = jnp.concatenate(
        [
            jnp.concatenate(
                [table[32 * slab : 32 * slab + 16], table[32 * slab + 16 : 32 * slab + 32]], axis=1
            )
            for slab in range(8)
        ],
        axis=0,
    )
    halved = dot(packed, wide, ((1,), (1,))).astype(BF16)
    for slab in range(8):
        out_ref[slab, pl.ds(MODES * PAIRS, 16), :] = halved[16 * slab : 16 * (slab + 1)]
    for pair in range(PAIRS):
        if pair % 2 == 0:
            copies[2 + pair // 2].wait()
        rows = forcing_ref[pl.ds(128 * pair, 128), :]
        halved = dot(table, rows, ((1,), (1,))).astype(BF16)
        for slab in range(8):
            out_ref[slab, pl.ds(MODES * pair, MODES), :] = halved[MODES * slab : MODES * (slab + 1)]


def source_kernel(
    turned_ref, table_ref, column_ref, row_ref, sources_ref, sums_ref, start_ref, local_ref
):
    gain, quad, mid, top = gains(slab_rates(column_ref, row_ref))
    for core in range(2):
        rows = MODES * PAIRS + (16 if core == 0 else 0)
        lhs = jnp.concatenate(
            [turned_ref[4 * core + y, pl.ds(0, rows), :] for y in range(4)], axis=1
        )
        spectra = dot(lhs, table_ref[...], ((1,), (0,)))
        for pair in range(PAIRS):
            for parity in range(2):
                part = spectra[
                    MODES * pair : MODES * (pair + 1), GRID * parity : GRID * (parity + 1)
                ]
                sources_ref[STEPS * core + 2 * pair + parity] = gain * part
        if core == 0:
            last = spectra[MODES * PAIRS :]
            start_ref[...] = jnp.concatenate([last[:, :GRID], last[:, GRID:]], axis=0)
    sums = []
    for point in range(CPOINTS):
        total = sources_ref[FINE_FACTOR * point]
        for step in range(1, FINE_FACTOR):
            total = gain * total + sources_ref[FINE_FACTOR * point + step]
        sums_ref[point] = total
        sums.append(total)
    begin = jnp.where(at_start(), start_ref[...], 0.0)
    leaving, _, _ = two_iterations((begin, None, begin, None), begin, sums, quad, mid, top)
    for index, array in enumerate(leaving):
        for side in range(2):
            local_ref[pl.ds(4 * side + index, MODES, stride=8), :] = array[
                :, 128 * side : 128 * (side + 1)
            ]


def scan_kernel(local_ref, column_ref, row_ref, state_ref):
    chip = lax.axis_index("tm_0") * 16 + lax.axis_index("tm_1")
    column = column_ref[pl.ds(mode_slab() * MODES + chip // 2, 1), :]
    row = jnp.where(chip % 2 == 0, row_ref[:, :128], row_ref[:, 128:])
    _, quad, mid, top = gains(column + row)
    units = []
    for index in range(3):
        state = [None] * 4
        state[index] = jnp.ones_like(top)
        units.append(two_iterations(state, None, [None] * CPOINTS, quad, mid, top)[0])
    power = top
    for _ in range(1, TOPS):
        power = power * top
    relaxed = error = relaxed2 = error2 = jnp.zeros_like(top)
    for block in range(BLOCKS):
        for index, array in enumerate((relaxed, error, relaxed2, error2)):
            state_ref[pl.ds(4 * block + index, 1), :] = array
        local = [local_ref[pl.ds(4 * block + index, 1), :] for index in range(4)]
        error2 = power * error2 + (
            local[3] + units[0][3] * relaxed + units[1][3] * error + units[2][3] * relaxed2
        )
        relaxed2 = units[1][2] * error + (local[2] + units[0][2] * relaxed)
        error = power * error + (local[1] + units[0][1] * relaxed)
        relaxed = local[0]


def path_kernel(
    state_ref, sources_ref, sums_ref, start_ref, high_ref, low_ref, column_ref, row_ref, out_ref
):
    gain, quad, mid, top = gains(slab_rates(column_ref, row_ref))
    state = [
        jnp.concatenate(
            [state_ref[pl.ds(4 * side + index, MODES, stride=8), :] for side in range(2)], axis=1
        )
        for index in range(4)
    ]
    first = at_start()
    start = start_ref[...]
    begin = jnp.where(first, start, 0.0)
    state[0] = jnp.where(first, start, state[0])
    state[2] = jnp.where(first, start, state[2])
    sums = [sums_ref[point] for point in range(CPOINTS)]
    _, one, two = two_iterations(state, begin, sums, quad, mid, top)

    def square_sum(array):
        column = jnp.sum(array * array, axis=0, keepdims=True)
        return jnp.sum(column[:, :128] + column[:, 128:], axis=1, keepdims=True)

    lane = lax.broadcasted_iota(jnp.int32, (1, 128), 1)
    for core in range(2):
        lines = []
        for kind in range(3):
            for which in (one, two):
                line = jnp.zeros((1, 128), F32)
                for point in range(4):
                    total = square_sum(which[kind][4 * core + point])
                    line = jnp.where(lane % 4 == point, total, line)
                lines.append(line)
        lines = jnp.concatenate(lines + [jnp.zeros((10, 128), F32)], axis=0)
        upper = lines.astype(BF16).astype(F32)
        rest = lines - upper
        middle = rest.astype(BF16).astype(F32)
        group = lax.broadcasted_iota(jnp.int32, (16, 128), 1) // 4
        packed = jnp.where(
            group == 0,
            upper,
            jnp.where(group == 1, middle, jnp.where(group == 2, rest - middle, 0.0)),
        ).astype(BF16)
        for y in range(4):
            out_ref[4 * core + y, pl.ds(MODES * PAIRS, 16), :] = packed

    before = [state[2] + state[3]] + two[2][:-1]
    for core in range(2):
        rows = []
        for point in range(4 * core, 4 * core + 4):
            current, visited = before[point], []
            for step in range(FINE_FACTOR - 1):
                current = gain * current + sources_ref[FINE_FACTOR * point + step]
                visited.append(current)
            visited.append(two[2][point])
            rows.append(jnp.concatenate(visited[:2], axis=1))
            rows.append(jnp.concatenate(visited[2:], axis=1))
        path = jnp.concatenate(rows, axis=0)
        high = path.astype(BF16)
        low = (path - high.astype(F32)).astype(BF16)
        turned = dot(high, high_ref[...], ((1,), (0,)))
        turned += dot(high, low_ref[...], ((1,), (0,)))
        turned += dot(low, high_ref[...], ((1,), (0,)))
        turned = turned.astype(BF16)
        for y in range(4):
            out_ref[4 * core + y, pl.ds(0, MODES * PAIRS), :] = turned[:, 128 * y : 128 * (y + 1)]


def heat_kernel(rows_ref, table_ref, heat_ref, history_ref, change_ref):
    table = table_ref[...]
    for pair in range(PAIRS):
        lhs = jnp.concatenate(
            [rows_ref[slab, pl.ds(MODES * pair, MODES), :] for slab in range(8)], axis=0
        )
        heat_ref[pl.ds(128 * pair, 128), :] = dot(lhs, table, ((0,), (0,)))
    total = jnp.zeros((16, 128), F32)
    for slab in range(8):
        total += rows_ref[slab, pl.ds(MODES * PAIRS, 16), :].astype(F32)
    total = total[:, 0:4] + total[:, 4:8] + total[:, 8:12]
    history_ref[...] = jnp.sqrt(total[0:2] / (GRID * GRID))
    change_ref[...] = jnp.sqrt(total[2:4] / total[4:6])


def call(kernel, outs, name):
    single = not isinstance(outs, (list, tuple))
    return pl.pallas_call(
        kernel,
        out_shape=outs if single else tuple(outs),
        compiler_params=pltpu.CompilerParams(vmem_limit_bytes=40 * 1024 * 1024),
        name=name,
    )


def per_device(forcing, starting_heat):
    half, inward, out_high, out_low = (jnp.asarray(c) for c in constants())
    mu = eigenvalues()
    columns = jnp.asarray(np.ascontiguousarray(np.broadcast_to(mu[:, None], (GRID, 128))))
    row = jnp.asarray(mu[None, :])
    shape = jax.ShapeDtypeStruct
    extent = MODES * PAIRS + 16
    ring = ("tm_2", "space")
    plane = ("tm_0", "tm_1")

    halved = pl.pallas_call(
        half_kernel,
        out_shape=shape((8, extent, 128), BF16),
        in_specs=[pl.BlockSpec(memory_space=pltpu.HBM)] * 3,
        scratch_shapes=[
            pltpu.VMEM((STEPS * SLAB, GRID), BF16),
            pltpu.VMEM((SLAB, GRID), BF16),
            pltpu.VMEM((GRID, GRID), BF16),
            pltpu.SemaphoreType.DMA((6,)),
        ],
        compiler_params=pltpu.CompilerParams(vmem_limit_bytes=66428928),
        name="half",
    )(forcing.reshape(STEPS * SLAB, GRID), starting_heat, half)
    turned = lax.all_to_all(halved, ring, 0, 0, tiled=True)
    sources, sums, start, local = call(
        source_kernel,
        [
            shape((2 * STEPS, MODES, GRID), F32),
            shape((CPOINTS, MODES, GRID), F32),
            shape((MODES, GRID), F32),
            shape((4 * BLOCKS, 128), F32),
        ],
        "source",
    )(turned, inward, columns, row)
    gathered = lax.all_to_all(local.reshape(BLOCKS, 4, 128), plane, 0, 0, tiled=True)
    states = call(scan_kernel, shape((4 * BLOCKS, 128), F32), "scan")(
        gathered.reshape(4 * BLOCKS, 128), columns, row
    )
    state = lax.all_to_all(states.reshape(BLOCKS, 4, 128), plane, 0, 0, tiled=True)
    rows = call(path_kernel, shape((8, extent, 128), BF16), "path")(
        state.reshape(4 * BLOCKS, 128), sources, sums, start, out_high, out_low, columns, row
    )
    returned = lax.all_to_all(rows, ring, 0, 0, tiled=True)
    heat, history, change = call(
        heat_kernel,
        [shape((STEPS * SLAB, GRID), F32), shape((2, 4), F32), shape((2, 4), F32)],
        "heat",
    )(returned, half)
    return heat.reshape(STEPS, SLAB, GRID), history, change


def solution(mesh):
    torus = Mesh(
        mesh.devices.reshape(4, 16, 2, mesh.shape["space"]), ("tm_0", "tm_1", "tm_2", "space")
    )
    tm = ("tm_0", "tm_1", "tm_2")
    in_specs = (P(tm, "space", None), P("space", None))
    out_specs = (P(tm, "space", None), P(None, tm), P(None, tm))
    return jax.shard_map(
        per_device, mesh=torus, in_specs=in_specs, out_specs=out_specs, check_vma=False
    )
```

```python
import functools
import math

import jax
import jax.numpy as jnp
import numpy as np
from jax import lax
from jax.experimental import pallas as pl
from jax.experimental.pallas import tpu as pltpu
from jax.sharding import Mesh
from jax.sharding import PartitionSpec as P

FINE_FACTOR = 4
COARSE_FACTOR = 4
DURATION = 0.004
GRID = 256
NT = 2048
SLAB = 64
MODES = 32
STEPS = 16
PAIRS = STEPS // 2
TOPS = 2
CPOINTS = TOPS * COARSE_FACTOR
BLOCKS = 64
PLANE_ORDER = [((x + 2) % 4) * 16 + (z + 8) % 16 for x in range(4) for z in range(16)]
RING_ORDER = [core * 4 + (y + 2) % 4 for core in range(2) for y in range(4)]
F32, BF16 = jnp.float32, jnp.bfloat16


def sine_table():
    numbers = np.arange(1, GRID + 1)
    product = numbers[:, None] * numbers[None, :] % (2 * (GRID + 1))
    angles = np.float32(np.pi) * product.astype(np.float32) / np.float32(GRID + 1)
    sines = np.sin(angles.astype(np.float64)).astype(np.float32)
    return np.float32(math.sqrt(2.0 / (GRID + 1))) * sines


def eigenvalues():
    halves = np.sin(np.pi * np.arange(1, GRID + 1) / (2 * (GRID + 1)))
    return (4.0 * (GRID + 1) ** 2 * halves * halves).astype(np.float32)


def constants():
    full = sine_table()
    half = full.astype(jnp.bfloat16)
    high = full.astype(jnp.bfloat16)
    low = (full - high.astype(np.float32)).astype(jnp.bfloat16)
    inward = np.zeros((4, 2, SLAB, 2, GRID), jnp.bfloat16)
    out_high = np.zeros((2, GRID, 4, 2, SLAB), jnp.bfloat16)
    out_low = np.zeros((2, GRID, 4, 2, SLAB), jnp.bfloat16)
    for k in range(2):
        inward[:, k, :, k, :] = half.reshape(4, SLAB, GRID)
        out_high[k, :, :, k, :] = high.reshape(GRID, 4, SLAB)
        out_low[k, :, :, k, :] = low.reshape(GRID, 4, SLAB)
    wide = 2 * GRID
    return (
        half,
        inward.reshape(wide, wide),
        out_high.reshape(wide, wide),
        out_low.reshape(wide, wide),
    )


def mul(a, b):
    return None if a is None or b is None else a * b


def add(a, b):
    return b if a is None else a if b is None else a + b


def sub(a, b):
    if b is None:
        return a
    return -b if a is None else a - b


def gains(rates):
    step = DURATION / NT
    gain = 1.0 / (1.0 + step * rates)
    mid = 1.0 / (1.0 + FINE_FACTOR * step * rates)
    top = 1.0 / (1.0 + FINE_FACTOR * COARSE_FACTOR * step * rates)
    square = gain * gain
    return gain, square * square, mid, top


def coarse_pass(entering, residual, mid, top):
    corrections = []
    for first in range(0, len(residual), COARSE_FACTOR):
        rows = residual[first : first + COARSE_FACTOR]
        running, inside = rows[0], entering
        for column in range(1, COARSE_FACTOR):
            inside = add(mul(mid, inside), rows[column - 1])
            corrections.append(inside)
            running = add(mul(mid, running), rows[column])
        entering = add(mul(top, entering), running)
        corrections.append(entering)
    return corrections, entering


def two_iterations(state, first_value, sums, quad, mid, top):
    relaxed_in, error_in, relaxed2_in, error2_in = state
    count = len(sums)
    relaxed = [add(mul(quad, first_value), sums[0])] + list(sums[1:])
    residual = [mul(quad, sub(relaxed_in, first_value))]
    residual += [mul(quad, relaxed[c - 1]) for c in range(1, count)]
    fix, error_out = coarse_pass(error_in, residual, mid, top)
    values = [add(r, p) for r, p in zip(relaxed, fix)]
    before = [add(relaxed_in, error_in)] + values[:-1]
    relaxed2 = [add(mul(quad, v), s) for v, s in zip(before, sums)]
    residual2 = [
        mul(quad, sub(r, v)) for r, v in zip([relaxed2_in] + relaxed2[:-1], before)
    ]
    fix2, error2_out = coarse_pass(error2_in, residual2, mid, top)
    values2 = [add(r, p) for r, p in zip(relaxed2, fix2)]
    leaving = (relaxed[-1], error_out, relaxed2[-1], error2_out)
    return leaving, (residual, fix, values), (residual2, fix2, values2)


def at_start():
    return jnp.logical_and(lax.axis_index("tm_0") == 0, lax.axis_index("tm_1") == 0)


def mode_slab():
    return lax.axis_index("tm_2") * 4 + (lax.axis_index("space") + 2) % 4


def exchange(array, axes, order):
    return lax.all_to_all(array, axes, 0, 0, axis_index_groups=[order], tiled=True)


def slab_rates(column_ref, row_ref):
    first = pl.multiple_of(mode_slab() * MODES, MODES)
    columns = column_ref[pl.ds(first, MODES), :]
    return jnp.concatenate([columns, columns], axis=1) + row_ref[...]


def dot(a, b, dims):
    return lax.dot_general(a, b, (dims, ((), ())), preferred_element_type=F32)


def half_kernel(
    forcing_hbm, start_hbm, table_hbm, out_ref, forcing_ref, start_ref, table_ref, arrived
):
    copies = [
        pltpu.make_async_copy(table_hbm, table_ref, arrived.at[0]),
        pltpu.make_async_copy(start_hbm, start_ref, arrived.at[1]),
    ]
    parts = 4
    rows = STEPS * SLAB // parts
    for part in range(parts):
        span = pl.ds(part * rows, rows)
        copies.append(
            pltpu.make_async_copy(
                forcing_hbm.at[span, :], forcing_ref.at[span, :], arrived.at[2 + part]
            )
        )
    for copy in copies:
        copy.start()
    copies[0].wait()
    copies[1].wait()
    table = table_ref[...]
    start = start_ref[...]
    nothing = jnp.zeros_like(start)
    wide = jnp.concatenate(
        [
            jnp.concatenate([start, nothing], axis=1),
            jnp.concatenate([nothing, start], axis=1),
        ],
        axis=0,
    )
    packed = jnp.concatenate(
        [
            jnp.concatenate(
                [table[32 * slab : 32 * slab + 16], table[32 * slab + 16 : 32 * slab + 32]], axis=1
            )
            for slab in range(8)
        ],
        axis=0,
    )
    halved = dot(packed, wide, ((1,), (1,))).astype(BF16)
    for slab in range(8):
        out_ref[slab, pl.ds(MODES * PAIRS, 16), :] = halved[16 * slab : 16 * (slab + 1)]
    for pair in range(PAIRS):
        if pair % 2 == 0:
            copies[2 + pair // 2].wait()
        rows = forcing_ref[pl.ds(128 * pair, 128), :]
        halved = dot(table, rows, ((1,), (1,))).astype(BF16)
        for slab in range(8):
            out_ref[slab, pl.ds(MODES * pair, MODES), :] = halved[MODES * slab : MODES * (slab + 1)]


def source_kernel(
    turned_ref, table_ref, column_ref, row_ref, sources_ref, sums_ref, start_ref, local_ref
):
    gain, quad, mid, top = gains(slab_rates(column_ref, row_ref))
    for core in range(2):
        rows = MODES * PAIRS + (16 if core == 0 else 0)
        lhs = jnp.concatenate(
            [turned_ref[4 * core + (y + 2) % 4, pl.ds(0, rows), :] for y in range(4)], axis=1
        )
        spectra = dot(lhs, table_ref[...], ((1,), (0,)))
        for pair in range(PAIRS):
            for parity in range(2):
                part = spectra[
                    MODES * pair : MODES * (pair + 1), GRID * parity : GRID * (parity + 1)
                ]
                sources_ref[STEPS * core + 2 * pair + parity] = gain * part
        if core == 0:
            last = spectra[MODES * PAIRS :]
            start_ref[...] = jnp.concatenate([last[:, :GRID], last[:, GRID:]], axis=0)
    sums = []
    for point in range(CPOINTS):
        total = sources_ref[FINE_FACTOR * point]
        for step in range(1, FINE_FACTOR):
            total = gain * total + sources_ref[FINE_FACTOR * point + step]
        sums_ref[point] = total
        sums.append(total)
    begin = jnp.where(at_start(), start_ref[...], 0.0)
    leaving, _, _ = two_iterations((begin, None, begin, None), begin, sums, quad, mid, top)
    for index, array in enumerate(leaving):
        for side in range(2):
            local_ref[pl.ds(4 * side + index, MODES, stride=8), :] = array[
                :, 128 * side : 128 * (side + 1)
            ]


def scan_kernel(local_ref, column_ref, row_ref, state_ref):
    chip = (lax.axis_index("tm_0") + 2) % 4 * 16 + (lax.axis_index("tm_1") + 8) % 16
    column = column_ref[pl.ds(mode_slab() * MODES + chip // 2, 1), :]
    row = jnp.where(chip % 2 == 0, row_ref[:, :128], row_ref[:, 128:])
    _, quad, mid, top = gains(column + row)
    units = []
    for index in range(3):
        state = [None] * 4
        state[index] = jnp.ones_like(top)
        units.append(two_iterations(state, None, [None] * CPOINTS, quad, mid, top)[0])
    power = top
    for _ in range(1, TOPS):
        power = power * top
    relaxed = error = relaxed2 = error2 = jnp.zeros_like(top)
    for block in range(BLOCKS):
        place = PLANE_ORDER.index(block)
        for index, array in enumerate((relaxed, error, relaxed2, error2)):
            state_ref[pl.ds(4 * place + index, 1), :] = array
        local = [local_ref[pl.ds(4 * place + index, 1), :] for index in range(4)]
        error2 = power * error2 + (
            local[3] + units[0][3] * relaxed + units[1][3] * error + units[2][3] * relaxed2
        )
        relaxed2 = units[1][2] * error + (local[2] + units[0][2] * relaxed)
        error = power * error + (local[1] + units[0][1] * relaxed)
        relaxed = local[0]


def path_kernel(
    state_ref, sources_ref, sums_ref, start_ref, high_ref, low_ref, column_ref, row_ref, out_ref
):
    gain, quad, mid, top = gains(slab_rates(column_ref, row_ref))
    state = [
        jnp.concatenate(
            [state_ref[pl.ds(4 * side + index, MODES, stride=8), :] for side in range(2)], axis=1
        )
        for index in range(4)
    ]
    first = at_start()
    start = start_ref[...]
    begin = jnp.where(first, start, 0.0)
    state[0] = jnp.where(first, start, state[0])
    state[2] = jnp.where(first, start, state[2])
    sums = [sums_ref[point] for point in range(CPOINTS)]
    _, one, two = two_iterations(state, begin, sums, quad, mid, top)

    def square_sum(array):
        column = jnp.sum(array * array, axis=0, keepdims=True)
        return jnp.sum(column[:, :128] + column[:, 128:], axis=1, keepdims=True)

    lane = lax.broadcasted_iota(jnp.int32, (1, 128), 1)
    for core in range(2):
        lines = []
        for kind in range(3):
            for which in (one, two):
                line = jnp.zeros((1, 128), F32)
                for point in range(4):
                    total = square_sum(which[kind][4 * core + point])
                    line = jnp.where(lane % 4 == point, total, line)
                lines.append(line)
        lines = jnp.concatenate(lines + [jnp.zeros((10, 128), F32)], axis=0)
        upper = lines.astype(BF16).astype(F32)
        rest = lines - upper
        middle = rest.astype(BF16).astype(F32)
        group = lax.broadcasted_iota(jnp.int32, (16, 128), 1) // 4
        packed = jnp.where(
            group == 0,
            upper,
            jnp.where(group == 1, middle, jnp.where(group == 2, rest - middle, 0.0)),
        ).astype(BF16)
        for y in range(4):
            out_ref[4 * core + y, pl.ds(MODES * PAIRS, 16), :] = packed

    before = [state[2] + state[3]] + two[2][:-1]
    for core in range(2):
        rows = []
        for point in range(4 * core, 4 * core + 4):
            current, visited = before[point], []
            for step in range(FINE_FACTOR - 1):
                current = gain * current + sources_ref[FINE_FACTOR * point + step]
                visited.append(current)
            visited.append(two[2][point])
            rows.append(jnp.concatenate(visited[:2], axis=1))
            rows.append(jnp.concatenate(visited[2:], axis=1))
        path = jnp.concatenate(rows, axis=0)
        high = path.astype(BF16)
        low = (path - high.astype(F32)).astype(BF16)
        turned = dot(high, high_ref[...], ((1,), (0,)))
        turned += dot(high, low_ref[...], ((1,), (0,)))
        turned += dot(low, high_ref[...], ((1,), (0,)))
        turned = turned.astype(BF16)
        for y in range(4):
            place = 4 * core + (y + 2) % 4
            out_ref[place, pl.ds(0, MODES * PAIRS), :] = turned[:, 128 * y : 128 * (y + 1)]


def heat_kernel(rows_ref, table_ref, heat_ref, history_ref, change_ref):
    table = table_ref[...]
    for pair in range(PAIRS):
        lhs = jnp.concatenate(
            [rows_ref[slab, pl.ds(MODES * pair, MODES), :] for slab in range(8)], axis=0
        )
        heat_ref[pl.ds(128 * pair, 128), :] = dot(lhs, table, ((0,), (0,)))
    total = jnp.zeros((16, 128), F32)
    for slab in range(8):
        total += rows_ref[slab, pl.ds(MODES * PAIRS, 16), :].astype(F32)
    total = total[:, 0:4] + total[:, 4:8] + total[:, 8:12]
    history_ref[...] = jnp.sqrt(total[0:2] / (GRID * GRID))
    change_ref[...] = jnp.sqrt(total[2:4] / total[4:6])


def call(kernel, outs, name):
    single = not isinstance(outs, (list, tuple))
    return pl.pallas_call(
        kernel,
        out_shape=outs if single else tuple(outs),
        compiler_params=pltpu.CompilerParams(vmem_limit_bytes=40 * 1024 * 1024),
        name=name,
    )


def per_device(forcing, starting_heat):
    half, inward, out_high, out_low = (jnp.asarray(c) for c in constants())
    mu = eigenvalues()
    columns = jnp.asarray(np.ascontiguousarray(np.broadcast_to(mu[:, None], (GRID, 128))))
    row = jnp.asarray(mu[None, :])
    shape = jax.ShapeDtypeStruct
    extent = MODES * PAIRS + 16
    ring = ("tm_2", "space")
    plane = ("tm_0", "tm_1")

    halved = pl.pallas_call(
        half_kernel,
        out_shape=shape((8, extent, 128), BF16),
        in_specs=[pl.BlockSpec(memory_space=pltpu.HBM)] * 3,
        scratch_shapes=[
            pltpu.VMEM((STEPS * SLAB, GRID), BF16),
            pltpu.VMEM((SLAB, GRID), BF16),
            pltpu.VMEM((GRID, GRID), BF16),
            pltpu.SemaphoreType.DMA((6,)),
        ],
        compiler_params=pltpu.CompilerParams(vmem_limit_bytes=66428928),
        name="half",
    )(forcing.reshape(STEPS * SLAB, GRID), starting_heat, half)
    turned = exchange(halved, ring, RING_ORDER)
    sources, sums, start, local = call(
        source_kernel,
        [
            shape((2 * STEPS, MODES, GRID), F32),
            shape((CPOINTS, MODES, GRID), F32),
            shape((MODES, GRID), F32),
            shape((4 * BLOCKS, 128), F32),
        ],
        "source",
    )(turned, inward, columns, row)
    gathered = exchange(local.reshape(BLOCKS, 4, 128), plane, PLANE_ORDER)
    states = call(scan_kernel, shape((4 * BLOCKS, 128), F32), "scan")(
        gathered.reshape(4 * BLOCKS, 128), columns, row
    )
    state = exchange(states.reshape(BLOCKS, 4, 128), plane, PLANE_ORDER)
    rows = call(path_kernel, shape((8, extent, 128), BF16), "path")(
        state.reshape(4 * BLOCKS, 128), sources, sums, start, out_high, out_low, columns, row
    )
    returned = exchange(rows, ring, RING_ORDER)
    heat, history, change = call(
        heat_kernel,
        [shape((STEPS * SLAB, GRID), F32), shape((2, 4), F32), shape((2, 4), F32)],
        "heat",
    )(returned, half)
    return heat.reshape(STEPS, SLAB, GRID), history, change


def solution(mesh):
    torus = Mesh(
        mesh.devices.reshape(4, 16, 2, mesh.shape["space"]), ("tm_0", "tm_1", "tm_2", "space")
    )
    tm = ("tm_0", "tm_1", "tm_2")
    in_specs = (P(tm, "space", None), P("space", None))
    out_specs = (P(tm, "space", None), P(None, tm), P(None, tm))
    return jax.shard_map(
        per_device, mesh=torus, in_specs=in_specs, out_specs=out_specs, check_vma=False
    )
```

```python
import functools
import math

import jax
import jax.numpy as jnp
import numpy as np
from jax import lax
from jax.experimental import pallas as pl
from jax.experimental.pallas import tpu as pltpu
from jax.sharding import Mesh
from jax.sharding import PartitionSpec as P

FINE_FACTOR = 4
COARSE_FACTOR = 4
DURATION = 0.004
GRID = 256
NT = 2048
SLAB = 64
MODES = 32
STEPS = 16
PAIRS = STEPS // 2
TOPS = 2
HEAT_PARTS = 4
CPOINTS = TOPS * COARSE_FACTOR
BLOCKS = 64
PLANE_ORDER = [((x + 2) % 4) * 16 + (z + 8) % 16 for x in range(4) for z in range(16)]
RING_ORDER = [core * 4 + (y + 2) % 4 for core in range(2) for y in range(4)]
F32, BF16 = jnp.float32, jnp.bfloat16


def sine_table():
    numbers = np.arange(1, GRID + 1)
    product = numbers[:, None] * numbers[None, :] % (2 * (GRID + 1))
    angles = np.float32(np.pi) * product.astype(np.float32) / np.float32(GRID + 1)
    sines = np.sin(angles.astype(np.float64)).astype(np.float32)
    return np.float32(math.sqrt(2.0 / (GRID + 1))) * sines


def eigenvalues():
    halves = np.sin(np.pi * np.arange(1, GRID + 1) / (2 * (GRID + 1)))
    return (4.0 * (GRID + 1) ** 2 * halves * halves).astype(np.float32)


def constants():
    full = sine_table()
    half = full.astype(jnp.bfloat16)
    low = (full - half.astype(np.float32)).astype(jnp.bfloat16)
    inward = np.zeros((4, 2, SLAB, 2, GRID), jnp.bfloat16)
    for k in range(2):
        inward[:, k, :, k, :] = half.reshape(4, SLAB, GRID)
    wide = 2 * GRID
    return half, low, inward.reshape(wide, wide)


def mul(a, b):
    return None if a is None or b is None else a * b


def add(a, b):
    return b if a is None else a if b is None else a + b


def sub(a, b):
    if b is None:
        return a
    return -b if a is None else a - b


def gains(rates):
    step = DURATION / NT
    gain = 1.0 / (1.0 + step * rates)
    mid = 1.0 / (1.0 + FINE_FACTOR * step * rates)
    top = 1.0 / (1.0 + FINE_FACTOR * COARSE_FACTOR * step * rates)
    square = gain * gain
    return gain, square * square, mid, top


def coarse_pass(entering, residual, mid, top):
    corrections = []
    for first in range(0, len(residual), COARSE_FACTOR):
        rows = residual[first : first + COARSE_FACTOR]
        running, inside = rows[0], entering
        for column in range(1, COARSE_FACTOR):
            inside = add(mul(mid, inside), rows[column - 1])
            corrections.append(inside)
            running = add(mul(mid, running), rows[column])
        entering = add(mul(top, entering), running)
        corrections.append(entering)
    return corrections, entering


def two_iterations(state, first_value, sums, quad, mid, top):
    relaxed_in, error_in, relaxed2_in, error2_in = state
    count = len(sums)
    relaxed = [add(mul(quad, first_value), sums[0])] + list(sums[1:])
    residual = [mul(quad, sub(relaxed_in, first_value))]
    residual += [mul(quad, relaxed[c - 1]) for c in range(1, count)]
    fix, error_out = coarse_pass(error_in, residual, mid, top)
    values = [add(r, p) for r, p in zip(relaxed, fix)]
    before = [add(relaxed_in, error_in)] + values[:-1]
    relaxed2 = [add(mul(quad, v), s) for v, s in zip(before, sums)]
    residual2 = [
        mul(quad, sub(r, v)) for r, v in zip([relaxed2_in] + relaxed2[:-1], before)
    ]
    fix2, error2_out = coarse_pass(error2_in, residual2, mid, top)
    values2 = [add(r, p) for r, p in zip(relaxed2, fix2)]
    leaving = (relaxed[-1], error_out, relaxed2[-1], error2_out)
    return leaving, (residual, fix, values), (residual2, fix2, values2)


def at_start():
    return jnp.logical_and(lax.axis_index("tm_0") == 0, lax.axis_index("tm_1") == 0)


def mode_slab():
    return lax.axis_index("tm_2") * 4 + (lax.axis_index("space") + 2) % 4


def exchange(array, axes, order):
    return lax.all_to_all(array, axes, 0, 0, axis_index_groups=[order], tiled=True)


def slab_rates(column_ref, row_ref):
    first = pl.multiple_of(mode_slab() * MODES, MODES)
    columns = column_ref[pl.ds(first, MODES), :]
    return jnp.concatenate([columns, columns], axis=1) + row_ref[...]


def dot(a, b, dims):
    return lax.dot_general(a, b, (dims, ((), ())), preferred_element_type=F32)


def half_kernel(forcing_ref, start_ref, table_ref, out_ref):
    table = table_ref[...]
    start = start_ref[...]
    nothing = jnp.zeros_like(start)
    wide = jnp.concatenate(
        [
            jnp.concatenate([start, nothing], axis=1),
            jnp.concatenate([nothing, start], axis=1),
        ],
        axis=0,
    )
    packed = jnp.concatenate(
        [
            jnp.concatenate(
                [table[32 * slab : 32 * slab + 16], table[32 * slab + 16 : 32 * slab + 32]], axis=1
            )
            for slab in range(8)
        ],
        axis=0,
    )
    halved = dot(packed, wide, ((1,), (1,))).astype(BF16)
    for slab in range(8):
        out_ref[slab, pl.ds(MODES * PAIRS, 16), :] = halved[16 * slab : 16 * (slab + 1)]
    for pair in range(PAIRS):
        rows = forcing_ref[pl.ds(128 * pair, 128), :]
        halved = dot(table, rows, ((1,), (1,))).astype(BF16)
        for slab in range(8):
            out_ref[slab, pl.ds(MODES * pair, MODES), :] = halved[MODES * slab : MODES * (slab + 1)]


def source_kernel(
    turned_ref, table_ref, column_ref, row_ref, sources_ref, sums_ref, start_ref, local_ref
):
    gain, quad, mid, top = gains(slab_rates(column_ref, row_ref))
    for core in range(2):
        rows = MODES * PAIRS + (16 if core == 0 else 0)
        lhs = jnp.concatenate(
            [turned_ref[4 * core + (y + 2) % 4, pl.ds(0, rows), :] for y in range(4)], axis=1
        )
        spectra = dot(lhs, table_ref[...], ((1,), (0,)))
        for pair in range(PAIRS):
            for parity in range(2):
                part = spectra[
                    MODES * pair : MODES * (pair + 1), GRID * parity : GRID * (parity + 1)
                ]
                sources_ref[STEPS * core + 2 * pair + parity] = gain * part
        if core == 0:
            last = spectra[MODES * PAIRS :]
            start_ref[...] = jnp.concatenate([last[:, :GRID], last[:, GRID:]], axis=0)
    sums = []
    for point in range(CPOINTS):
        total = sources_ref[FINE_FACTOR * point]
        for step in range(1, FINE_FACTOR):
            total = gain * total + sources_ref[FINE_FACTOR * point + step]
        sums_ref[point] = total
        sums.append(total)
    begin = jnp.where(at_start(), start_ref[...], 0.0)
    leaving, _, _ = two_iterations((begin, None, begin, None), begin, sums, quad, mid, top)
    for index, array in enumerate(leaving):
        for side in range(2):
            local_ref[pl.ds(4 * side + index, MODES, stride=8), :] = array[
                :, 128 * side : 128 * (side + 1)
            ]


def scan_kernel(local_ref, column_ref, row_ref, state_ref):
    chip = (lax.axis_index("tm_0") + 2) % 4 * 16 + (lax.axis_index("tm_1") + 8) % 16
    column = column_ref[pl.ds(mode_slab() * MODES + chip // 2, 1), :]
    row = jnp.where(chip % 2 == 0, row_ref[:, :128], row_ref[:, 128:])
    _, quad, mid, top = gains(column + row)
    units = []
    for index in range(3):
        state = [None] * 4
        state[index] = jnp.ones_like(top)
        units.append(two_iterations(state, None, [None] * CPOINTS, quad, mid, top)[0])
    power = top
    for _ in range(1, TOPS):
        power = power * top
    relaxed = error = relaxed2 = error2 = jnp.zeros_like(top)
    for block in range(BLOCKS):
        place = PLANE_ORDER.index(block)
        for index, array in enumerate((relaxed, error, relaxed2, error2)):
            state_ref[pl.ds(4 * place + index, 1), :] = array
        local = [local_ref[pl.ds(4 * place + index, 1), :] for index in range(4)]
        error2 = power * error2 + (
            local[3] + units[0][3] * relaxed + units[1][3] * error + units[2][3] * relaxed2
        )
        relaxed2 = units[1][2] * error + (local[2] + units[0][2] * relaxed)
        error = power * error + (local[1] + units[0][1] * relaxed)
        relaxed = local[0]


def path_kernel(
    state_ref, sources_ref, sums_ref, start_ref, high_ref, low_ref, column_ref, row_ref, out_ref
):
    gain, quad, mid, top = gains(slab_rates(column_ref, row_ref))
    state = [
        jnp.concatenate(
            [state_ref[pl.ds(4 * side + index, MODES, stride=8), :] for side in range(2)], axis=1
        )
        for index in range(4)
    ]
    first = at_start()
    start = start_ref[...]
    begin = jnp.where(first, start, 0.0)
    state[0] = jnp.where(first, start, state[0])
    state[2] = jnp.where(first, start, state[2])
    sums = [sums_ref[point] for point in range(CPOINTS)]
    _, one, two = two_iterations(state, begin, sums, quad, mid, top)

    def square_sum(array):
        column = jnp.sum(array * array, axis=0, keepdims=True)
        return jnp.sum(column[:, :128] + column[:, 128:], axis=1, keepdims=True)

    lane = lax.broadcasted_iota(jnp.int32, (1, 128), 1)
    for core in range(2):
        lines = []
        for kind in range(3):
            for which in (one, two):
                line = jnp.zeros((1, 128), F32)
                for point in range(4):
                    total = square_sum(which[kind][4 * core + point])
                    line = jnp.where(lane % 4 == point, total, line)
                lines.append(line)
        lines = jnp.concatenate(lines + [jnp.zeros((10, 128), F32)], axis=0)
        upper = lines.astype(BF16).astype(F32)
        rest = lines - upper
        middle = rest.astype(BF16).astype(F32)
        group = lax.broadcasted_iota(jnp.int32, (16, 128), 1) // 4
        packed = jnp.where(
            group == 0,
            upper,
            jnp.where(group == 1, middle, jnp.where(group == 2, rest - middle, 0.0)),
        ).astype(BF16)
        for y in range(4):
            out_ref[4 * core + y, pl.ds(MODES * PAIRS, 16), :] = packed

    before = [state[2] + state[3]] + two[2][:-1]
    for core in range(2):
        rows = [[], []]
        for point in range(4 * core, 4 * core + 4):
            current = before[point]
            for step in range(FINE_FACTOR - 1):
                current = gain * current + sources_ref[FINE_FACTOR * point + step]
                rows[step % 2].append(current)
            rows[1].append(two[2][point])
        turned = []
        for parity in range(2):
            path = jnp.concatenate(rows[parity], axis=0)
            high = path.astype(BF16)
            low = (path - high.astype(F32)).astype(BF16)
            part = dot(high, high_ref[...], ((1,), (0,)))
            part += dot(high, low_ref[...], ((1,), (0,)))
            part += dot(low, high_ref[...], ((1,), (0,)))
            turned.append(part)
        left = lax.broadcasted_iota(jnp.int32, (MODES * PAIRS, 128), 1) < SLAB
        for group in range(2):
            even, odd = (part[:, 128 * group : 128 * (group + 1)] for part in turned)
            sides = (
                jnp.where(left, even, pltpu.roll(odd, SLAB, 1)),
                jnp.where(left, pltpu.roll(even, SLAB, 1), odd),
            )
            for side in range(2):
                place = 4 * core + (2 * group + side + 2) % 4
                out_ref[place, pl.ds(0, MODES * PAIRS), :] = sides[side].astype(BF16)


def heat_kernel(rows_ref, table_ref, heat_ref, history_ref, change_ref):
    table = table_ref[...]
    first = pl.program_id(0) * (PAIRS // HEAT_PARTS)
    for pair in range(PAIRS // HEAT_PARTS):
        span = pl.ds(pl.multiple_of(MODES * (first + pair), MODES), MODES)
        lhs = jnp.concatenate([rows_ref[slab, span, :] for slab in range(8)], axis=0)
        heat_ref[pl.ds(128 * pair, 128), :] = dot(lhs, table, ((0,), (0,)))
    total = jnp.zeros((16, 128), F32)
    for slab in range(8):
        total += rows_ref[slab, pl.ds(MODES * PAIRS, 16), :].astype(F32)
    total = total[:, 0:4] + total[:, 4:8] + total[:, 8:12]
    history_ref[...] = jnp.sqrt(total[0:2] / (GRID * GRID))
    change_ref[...] = jnp.sqrt(total[2:4] / total[4:6])


def call(kernel, outs, name):
    single = not isinstance(outs, (list, tuple))
    return pl.pallas_call(
        kernel,
        out_shape=outs if single else tuple(outs),
        compiler_params=pltpu.CompilerParams(vmem_limit_bytes=40 * 1024 * 1024),
        name=name,
    )


def per_device(forcing, starting_heat):
    half, low, inward = (jnp.asarray(c) for c in constants())
    mu = eigenvalues()
    columns = jnp.asarray(np.ascontiguousarray(np.broadcast_to(mu[:, None], (GRID, 128))))
    row = jnp.asarray(mu[None, :])
    shape = jax.ShapeDtypeStruct
    extent = MODES * PAIRS + 16
    ring = ("tm_2", "space")
    plane = ("tm_0", "tm_1")

    halved = call(half_kernel, shape((8, extent, 128), BF16), "half")(
        forcing.reshape(STEPS * SLAB, GRID), starting_heat, half
    )
    turned = exchange(halved, ring, RING_ORDER)
    sources, sums, start, local = call(
        source_kernel,
        [
            shape((2 * STEPS, MODES, GRID), F32),
            shape((CPOINTS, MODES, GRID), F32),
            shape((MODES, GRID), F32),
            shape((4 * BLOCKS, 128), F32),
        ],
        "source",
    )(turned, inward, columns, row)
    gathered = exchange(local.reshape(BLOCKS, 4, 128), plane, PLANE_ORDER)
    states = call(scan_kernel, shape((4 * BLOCKS, 128), F32), "scan")(
        gathered.reshape(4 * BLOCKS, 128), columns, row
    )
    state = exchange(states.reshape(BLOCKS, 4, 128), plane, PLANE_ORDER)
    rows = call(path_kernel, shape((8, extent, 128), BF16), "path")(
        state.reshape(4 * BLOCKS, 128), sources, sums, start, half, low, columns, row
    )
    returned = exchange(rows, ring, RING_ORDER)
    whole = pl.BlockSpec(memory_space=pltpu.VMEM)
    small = pl.BlockSpec((2, 4), lambda part: (0, 0))
    heat, history, change = pl.pallas_call(
        heat_kernel,
        grid=(HEAT_PARTS,),
        in_specs=[whole, whole],
        out_specs=[
            pl.BlockSpec((STEPS * SLAB // HEAT_PARTS, GRID), lambda part: (part, 0)),
            small,
            small,
        ],
        out_shape=(shape((STEPS * SLAB, GRID), F32), shape((2, 4), F32), shape((2, 4), F32)),
        compiler_params=pltpu.CompilerParams(vmem_limit_bytes=40 * 1024 * 1024),
        name="heat",
    )(returned, half)
    return heat.reshape(STEPS, SLAB, GRID), history, change


def solution(mesh):
    torus = Mesh(
        mesh.devices.reshape(4, 16, 2, mesh.shape["space"]), ("tm_0", "tm_1", "tm_2", "space")
    )
    tm = ("tm_0", "tm_1", "tm_2")
    in_specs = (P(tm, "space", None), P("space", None))
    out_specs = (P(tm, "space", None), P(None, tm), P(None, tm))
    return jax.shard_map(
        per_device, mesh=torus, in_specs=in_specs, out_specs=out_specs, check_vma=False
    )
```

```python
import functools
import math

import jax
import jax.numpy as jnp
import numpy as np
from jax import lax
from jax.experimental import pallas as pl
from jax.experimental.pallas import tpu as pltpu
from jax.sharding import Mesh
from jax.sharding import PartitionSpec as P

FINE_FACTOR = 4
COARSE_FACTOR = 4
DURATION = 0.004
GRID = 256
NT = 2048
SLAB = 64
MODES = 32
STEPS = 16
PAIRS = STEPS // 2
TOPS = 2
HEAT_PARTS = 4
CPOINTS = TOPS * COARSE_FACTOR
BLOCKS = 64
PLANE_ORDER = [((x + 2) % 4) * 16 + (z + 8) % 16 for x in range(4) for z in range(16)]
RING_ORDER = [core * 4 + (y + 2) % 4 for core in range(2) for y in range(4)]
F32, BF16 = jnp.float32, jnp.bfloat16


def sine_table():
    numbers = np.arange(1, GRID + 1)
    product = numbers[:, None] * numbers[None, :] % (2 * (GRID + 1))
    angles = np.float32(np.pi) * product.astype(np.float32) / np.float32(GRID + 1)
    sines = np.sin(angles.astype(np.float64)).astype(np.float32)
    return np.float32(math.sqrt(2.0 / (GRID + 1))) * sines


def eigenvalues():
    halves = np.sin(np.pi * np.arange(1, GRID + 1) / (2 * (GRID + 1)))
    return (4.0 * (GRID + 1) ** 2 * halves * halves).astype(np.float32)


def constants():
    full = sine_table()
    half = full.astype(jnp.bfloat16)
    low = (full - half.astype(np.float32)).astype(jnp.bfloat16)
    inward = np.zeros((4, 2, SLAB, 2, GRID), jnp.bfloat16)
    for k in range(2):
        inward[:, k, :, k, :] = half.reshape(4, SLAB, GRID)
    wide = 2 * GRID
    return half, low, inward.reshape(wide, wide)


def mul(a, b):
    return None if a is None or b is None else a * b


def add(a, b):
    return b if a is None else a if b is None else a + b


def sub(a, b):
    if b is None:
        return a
    return -b if a is None else a - b


def gains(rates):
    step = DURATION / NT
    gain = 1.0 / (1.0 + step * rates)
    mid = 1.0 / (1.0 + FINE_FACTOR * step * rates)
    top = 1.0 / (1.0 + FINE_FACTOR * COARSE_FACTOR * step * rates)
    square = gain * gain
    return gain, square * square, mid, top


def coarse_pass(entering, residual, mid, top):
    corrections = []
    for first in range(0, len(residual), COARSE_FACTOR):
        rows = residual[first : first + COARSE_FACTOR]
        running, inside = rows[0], entering
        for column in range(1, COARSE_FACTOR):
            inside = add(mul(mid, inside), rows[column - 1])
            corrections.append(inside)
            running = add(mul(mid, running), rows[column])
        entering = add(mul(top, entering), running)
        corrections.append(entering)
    return corrections, entering


def two_iterations(state, first_value, sums, quad, mid, top):
    relaxed_in, error_in, relaxed2_in, error2_in = state
    count = len(sums)
    relaxed = [add(mul(quad, first_value), sums[0])] + list(sums[1:])
    residual = [mul(quad, sub(relaxed_in, first_value))]
    residual += [mul(quad, relaxed[c - 1]) for c in range(1, count)]
    fix, error_out = coarse_pass(error_in, residual, mid, top)
    values = [add(r, p) for r, p in zip(relaxed, fix)]
    before = [add(relaxed_in, error_in)] + values[:-1]
    relaxed2 = [add(mul(quad, v), s) for v, s in zip(before, sums)]
    residual2 = [
        mul(quad, sub(r, v)) for r, v in zip([relaxed2_in] + relaxed2[:-1], before)
    ]
    fix2, error2_out = coarse_pass(error2_in, residual2, mid, top)
    values2 = [add(r, p) for r, p in zip(relaxed2, fix2)]
    leaving = (relaxed[-1], error_out, relaxed2[-1], error2_out)
    return leaving, (residual, fix, values), (residual2, fix2, values2)


def at_start():
    return jnp.logical_and(lax.axis_index("tm_0") == 0, lax.axis_index("tm_1") == 0)


def mode_slab():
    return lax.axis_index("tm_2") * 4 + (lax.axis_index("space") + 2) % 4


def exchange(array, axes, order):
    return lax.all_to_all(array, axes, 0, 0, axis_index_groups=[order], tiled=True)


def slab_rates(column_ref, row_ref):
    first = pl.multiple_of(mode_slab() * MODES, MODES)
    columns = column_ref[pl.ds(first, MODES), :]
    return jnp.concatenate([columns, columns], axis=1) + row_ref[...]


def dot(a, b, dims):
    return lax.dot_general(a, b, (dims, ((), ())), preferred_element_type=F32)


def half_kernel(forcing_ref, start_ref, table_ref, out_ref):
    table = table_ref[...]
    start = start_ref[...]
    nothing = jnp.zeros_like(start)
    wide = jnp.concatenate(
        [
            jnp.concatenate([start, nothing], axis=1),
            jnp.concatenate([nothing, start], axis=1),
        ],
        axis=0,
    )
    packed = jnp.concatenate(
        [
            jnp.concatenate(
                [table[32 * slab : 32 * slab + 16], table[32 * slab + 16 : 32 * slab + 32]], axis=1
            )
            for slab in range(8)
        ],
        axis=0,
    )
    halved = dot(packed, wide, ((1,), (1,))).astype(BF16)
    for slab in range(8):
        out_ref[slab, pl.ds(MODES * PAIRS, 16), :] = halved[16 * slab : 16 * (slab + 1)]
    for pair in range(PAIRS):
        rows = forcing_ref[pl.ds(128 * pair, 128), :]
        halved = dot(table, rows, ((1,), (1,))).astype(BF16)
        for slab in range(8):
            out_ref[slab, pl.ds(MODES * pair, MODES), :] = halved[MODES * slab : MODES * (slab + 1)]


def source_kernel(
    turned_ref, table_ref, column_ref, row_ref, sources_ref, sums_ref, start_ref, local_ref
):
    gain, quad, mid, top = gains(slab_rates(column_ref, row_ref))
    for core in range(2):
        rows = MODES * PAIRS + (16 if core == 0 else 0)
        lhs = jnp.concatenate(
            [turned_ref[4 * core + (y + 2) % 4, pl.ds(0, rows), :] for y in range(4)], axis=1
        )
        spectra = dot(lhs, table_ref[...], ((1,), (0,)))
        for pair in range(PAIRS):
            for parity in range(2):
                part = spectra[
                    MODES * pair : MODES * (pair + 1), GRID * parity : GRID * (parity + 1)
                ]
                sources_ref[STEPS * core + 2 * pair + parity] = gain * part
        if core == 0:
            last = spectra[MODES * PAIRS :]
            start_ref[...] = jnp.concatenate([last[:, :GRID], last[:, GRID:]], axis=0)
    sums = []
    for point in range(CPOINTS):
        total = sources_ref[FINE_FACTOR * point]
        for step in range(1, FINE_FACTOR):
            total = gain * total + sources_ref[FINE_FACTOR * point + step]
        sums_ref[point] = total
        sums.append(total)
    begin = jnp.where(at_start(), start_ref[...], 0.0)
    leaving, _, _ = two_iterations((begin, None, begin, None), begin, sums, quad, mid, top)
    for index, array in enumerate(leaving):
        for side in range(2):
            local_ref[pl.ds(4 * side + index, MODES, stride=8), :] = array[
                :, 128 * side : 128 * (side + 1)
            ]


def scan_kernel(local_ref, column_ref, row_ref, state_ref):
    chip = (lax.axis_index("tm_0") + 2) % 4 * 16 + (lax.axis_index("tm_1") + 8) % 16
    column = column_ref[pl.ds(mode_slab() * MODES + chip // 2, 1), :]
    row = jnp.where(chip % 2 == 0, row_ref[:, :128], row_ref[:, 128:])
    _, quad, mid, top = gains(column + row)
    units = []
    for index in range(3):
        state = [None] * 4
        state[index] = jnp.ones_like(top)
        units.append(two_iterations(state, None, [None] * CPOINTS, quad, mid, top)[0])
    power = top
    for _ in range(1, TOPS):
        power = power * top
    relaxed = error = relaxed2 = error2 = jnp.zeros_like(top)
    for block in range(BLOCKS):
        place = PLANE_ORDER.index(block)
        for index, array in enumerate((relaxed, error, relaxed2, error2)):
            state_ref[pl.ds(4 * place + index, 1), :] = array
        local = [local_ref[pl.ds(4 * place + index, 1), :] for index in range(4)]
        error2 = power * error2 + (
            local[3] + units[0][3] * relaxed + units[1][3] * error + units[2][3] * relaxed2
        )
        relaxed2 = units[1][2] * error + (local[2] + units[0][2] * relaxed)
        error = power * error + (local[1] + units[0][1] * relaxed)
        relaxed = local[0]


def path_kernel(
    state_ref, sources_ref, sums_ref, start_ref, high_ref, low_ref, column_ref, row_ref, out_ref
):
    gain, quad, mid, top = gains(slab_rates(column_ref, row_ref))
    state = [
        jnp.concatenate(
            [state_ref[pl.ds(4 * side + index, MODES, stride=8), :] for side in range(2)], axis=1
        )
        for index in range(4)
    ]
    first = at_start()
    start = start_ref[...]
    begin = jnp.where(first, start, 0.0)
    state[0] = jnp.where(first, start, state[0])
    state[2] = jnp.where(first, start, state[2])
    sums = [sums_ref[point] for point in range(CPOINTS)]
    _, one, two = two_iterations(state, begin, sums, quad, mid, top)

    def square_sum(array):
        column = jnp.sum(array * array, axis=0, keepdims=True)
        return jnp.sum(column[:, :128] + column[:, 128:], axis=1, keepdims=True)

    lane = lax.broadcasted_iota(jnp.int32, (1, 128), 1)
    for core in range(2):
        lines = []
        for kind in range(3):
            for which in (one, two):
                line = jnp.zeros((1, 128), F32)
                for point in range(4):
                    total = square_sum(which[kind][4 * core + point])
                    line = jnp.where(lane % 4 == point, total, line)
                lines.append(line)
        lines = jnp.concatenate(lines + [jnp.zeros((10, 128), F32)], axis=0)
        upper = lines.astype(BF16).astype(F32)
        rest = lines - upper
        middle = rest.astype(BF16).astype(F32)
        group = lax.broadcasted_iota(jnp.int32, (16, 128), 1) // 4
        packed = jnp.where(
            group == 0,
            upper,
            jnp.where(group == 1, middle, jnp.where(group == 2, rest - middle, 0.0)),
        ).astype(BF16)
        for y in range(4):
            out_ref[4 * core + y, pl.ds(MODES * PAIRS, 16), :] = packed

    before = [state[2] + state[3]] + two[2][:-1]
    for core in range(2):
        rows = [[], []]
        for point in range(4 * core, 4 * core + 4):
            current = before[point]
            for step in range(FINE_FACTOR - 1):
                current = gain * current + sources_ref[FINE_FACTOR * point + step]
                rows[step % 2].append(current)
            rows[1].append(two[2][point])
        turned = []
        for parity in range(2):
            path = jnp.concatenate(rows[parity], axis=0)
            high = path.astype(BF16)
            low = (path - high.astype(F32)).astype(BF16)
            part = dot(high, high_ref[...], ((1,), (0,)))
            part += dot(high, low_ref[...], ((1,), (0,)))
            part += dot(low, high_ref[...], ((1,), (0,)))
            turned.append(part)
        left = lax.broadcasted_iota(jnp.int32, (MODES * PAIRS, 128), 1) < SLAB
        for group in range(2):
            even, odd = (part[:, 128 * group : 128 * (group + 1)] for part in turned)
            sides = (
                jnp.where(left, even, pltpu.roll(odd, SLAB, 1)),
                jnp.where(left, pltpu.roll(even, SLAB, 1), odd),
            )
            for side in range(2):
                place = 4 * core + (2 * group + side + 2) % 4
                out_ref[place, pl.ds(0, MODES * PAIRS), :] = sides[side].astype(BF16)


def heat_kernel(rows_ref, table_ref, heat_hbm, history_ref, change_ref, heat_ref, left):
    table = table_ref[...]
    rows = STEPS * SLAB // HEAT_PARTS
    copies = []
    for part in range(HEAT_PARTS):
        for pair in range(PAIRS // HEAT_PARTS * part, PAIRS // HEAT_PARTS * (part + 1)):
            span = pl.ds(MODES * pair, MODES)
            lhs = jnp.concatenate([rows_ref[slab, span, :] for slab in range(8)], axis=0)
            heat_ref[pl.ds(128 * pair, 128), :] = dot(lhs, table, ((0,), (0,)))
        span = pl.ds(rows * part, rows)
        copies.append(
            pltpu.make_async_copy(heat_ref.at[span, :], heat_hbm.at[span, :], left.at[part])
        )
        copies[-1].start()
    total = jnp.zeros((16, 128), F32)
    for slab in range(8):
        total += rows_ref[slab, pl.ds(MODES * PAIRS, 16), :].astype(F32)
    total = total[:, 0:4] + total[:, 4:8] + total[:, 8:12]
    history_ref[...] = jnp.sqrt(total[0:2] / (GRID * GRID))
    change_ref[...] = jnp.sqrt(total[2:4] / total[4:6])
    for copy in copies:
        copy.wait()


def call(kernel, outs, name):
    single = not isinstance(outs, (list, tuple))
    return pl.pallas_call(
        kernel,
        out_shape=outs if single else tuple(outs),
        compiler_params=pltpu.CompilerParams(vmem_limit_bytes=40 * 1024 * 1024),
        name=name,
    )


def per_device(forcing, starting_heat):
    half, low, inward = (jnp.asarray(c) for c in constants())
    mu = eigenvalues()
    columns = jnp.asarray(np.ascontiguousarray(np.broadcast_to(mu[:, None], (GRID, 128))))
    row = jnp.asarray(mu[None, :])
    shape = jax.ShapeDtypeStruct
    extent = MODES * PAIRS + 16
    ring = ("tm_2", "space")
    plane = ("tm_0", "tm_1")

    numbers = lax.optimization_barrier(jnp.arange(1, GRID + 1, dtype=jnp.int32))
    angles = numbers[:, None] * numbers[None, :] % (2 * (GRID + 1))
    angles = jnp.pi * angles.astype(F32) / (GRID + 1)
    table = (math.sqrt(2.0 / (GRID + 1)) * jnp.sin(angles)).astype(BF16)
    halved = call(half_kernel, shape((8, extent, 128), BF16), "half")(
        forcing.reshape(STEPS * SLAB, GRID), starting_heat, table
    )
    turned = exchange(halved, ring, RING_ORDER)
    sources, sums, start, local = call(
        source_kernel,
        [
            shape((2 * STEPS, MODES, GRID), F32),
            shape((CPOINTS, MODES, GRID), F32),
            shape((MODES, GRID), F32),
            shape((4 * BLOCKS, 128), F32),
        ],
        "source",
    )(turned, inward, columns, row)
    gathered = exchange(local.reshape(BLOCKS, 4, 128), plane, PLANE_ORDER)
    states = call(scan_kernel, shape((4 * BLOCKS, 128), F32), "scan")(
        gathered.reshape(4 * BLOCKS, 128), columns, row
    )
    state = exchange(states.reshape(BLOCKS, 4, 128), plane, PLANE_ORDER)
    rows = call(path_kernel, shape((8, extent, 128), BF16), "path")(
        state.reshape(4 * BLOCKS, 128), sources, sums, start, half, low, columns, row
    )
    returned = exchange(rows, ring, RING_ORDER)
    whole = pl.BlockSpec(memory_space=pltpu.VMEM)
    heat, history, change = pl.pallas_call(
        heat_kernel,
        in_specs=[whole, whole],
        out_specs=[pl.BlockSpec(memory_space=pltpu.HBM), whole, whole],
        scratch_shapes=[
            pltpu.VMEM((STEPS * SLAB, GRID), F32),
            pltpu.SemaphoreType.DMA((HEAT_PARTS,)),
        ],
        out_shape=(shape((STEPS * SLAB, GRID), F32), shape((2, 4), F32), shape((2, 4), F32)),
        compiler_params=pltpu.CompilerParams(vmem_limit_bytes=40 * 1024 * 1024),
        name="heat",
    )(returned, half)
    return heat.reshape(STEPS, SLAB, GRID), history, change


def solution(mesh):
    torus = Mesh(
        mesh.devices.reshape(4, 16, 2, mesh.shape["space"]), ("tm_0", "tm_1", "tm_2", "space")
    )
    tm = ("tm_0", "tm_1", "tm_2")
    in_specs = (P(tm, "space", None), P("space", None))
    out_specs = (P(tm, "space", None), P(None, tm), P(None, tm))
    return jax.shard_map(
        per_device, mesh=torus, in_specs=in_specs, out_specs=out_specs, check_vma=False
    )
```

```python
import functools
import math

import jax
import jax.numpy as jnp
import numpy as np
from jax import lax
from jax.experimental import pallas as pl
from jax.experimental.pallas import tpu as pltpu
from jax.sharding import Mesh
from jax.sharding import PartitionSpec as P

FINE_FACTOR = 4
COARSE_FACTOR = 4
DURATION = 0.004
GRID = 256
NT = 2048
SLAB = 64
MODES = 32
STEPS = 16
PAIRS = STEPS // 2
TOPS = 2
CPOINTS = TOPS * COARSE_FACTOR
BLOCKS = 64
PLANE_ORDER = [((x + 2) % 4) * 16 + (z + 8) % 16 for x in range(4) for z in range(16)]
RING_ORDER = [core * 4 + (y + 2) % 4 for core in range(2) for y in range(4)]
F32, BF16 = jnp.float32, jnp.bfloat16


def sine_table():
    numbers = np.arange(1, GRID + 1)
    product = numbers[:, None] * numbers[None, :] % (2 * (GRID + 1))
    angles = np.float32(np.pi) * product.astype(np.float32) / np.float32(GRID + 1)
    sines = np.sin(angles.astype(np.float64)).astype(np.float32)
    return np.float32(math.sqrt(2.0 / (GRID + 1))) * sines


def eigenvalues():
    halves = np.sin(np.pi * np.arange(1, GRID + 1) / (2 * (GRID + 1)))
    return (4.0 * (GRID + 1) ** 2 * halves * halves).astype(np.float32)


def constants():
    full = sine_table()
    half = full.astype(jnp.bfloat16)
    low = (full - half.astype(np.float32)).astype(jnp.bfloat16)
    inward = np.zeros((4, 2, SLAB, 2, GRID), jnp.bfloat16)
    for k in range(2):
        inward[:, k, :, k, :] = half.reshape(4, SLAB, GRID)
    wide = 2 * GRID
    return half, low, inward.reshape(wide, wide)


def mul(a, b):
    return None if a is None or b is None else a * b


def add(a, b):
    return b if a is None else a if b is None else a + b


def sub(a, b):
    if b is None:
        return a
    return -b if a is None else a - b


def gains(rates):
    step = DURATION / NT
    gain = 1.0 / (1.0 + step * rates)
    mid = 1.0 / (1.0 + FINE_FACTOR * step * rates)
    top = 1.0 / (1.0 + FINE_FACTOR * COARSE_FACTOR * step * rates)
    square = gain * gain
    return gain, square * square, mid, top


def coarse_pass(entering, residual, mid, top):
    corrections = []
    for first in range(0, len(residual), COARSE_FACTOR):
        rows = residual[first : first + COARSE_FACTOR]
        running, inside = rows[0], entering
        for column in range(1, COARSE_FACTOR):
            inside = add(mul(mid, inside), rows[column - 1])
            corrections.append(inside)
            running = add(mul(mid, running), rows[column])
        entering = add(mul(top, entering), running)
        corrections.append(entering)
    return corrections, entering


def two_iterations(state, first_value, sums, quad, mid, top):
    relaxed_in, error_in, relaxed2_in, error2_in = state
    count = len(sums)
    relaxed = [add(mul(quad, first_value), sums[0])] + list(sums[1:])
    residual = [mul(quad, sub(relaxed_in, first_value))]
    residual += [mul(quad, relaxed[c - 1]) for c in range(1, count)]
    fix, error_out = coarse_pass(error_in, residual, mid, top)
    values = [add(r, p) for r, p in zip(relaxed, fix)]
    before = [add(relaxed_in, error_in)] + values[:-1]
    relaxed2 = [add(mul(quad, v), s) for v, s in zip(before, sums)]
    residual2 = [
        mul(quad, sub(r, v)) for r, v in zip([relaxed2_in] + relaxed2[:-1], before)
    ]
    fix2, error2_out = coarse_pass(error2_in, residual2, mid, top)
    values2 = [add(r, p) for r, p in zip(relaxed2, fix2)]
    leaving = (relaxed[-1], error_out, relaxed2[-1], error2_out)
    return leaving, (residual, fix, values), (residual2, fix2, values2)


def at_start():
    return jnp.logical_and(lax.axis_index("tm_0") == 0, lax.axis_index("tm_1") == 0)


def mode_slab():
    return lax.axis_index("tm_2") * 4 + (lax.axis_index("space") + 2) % 4


def exchange(array, axes, order):
    return lax.all_to_all(array, axes, 0, 0, axis_index_groups=[order], tiled=True)


def slab_rates(column_ref, row_ref):
    first = pl.multiple_of(mode_slab() * MODES, MODES)
    columns = column_ref[pl.ds(first, MODES), :]
    return jnp.concatenate([columns, columns], axis=1) + row_ref[...]


def dot(a, b, dims):
    return lax.dot_general(a, b, (dims, ((), ())), preferred_element_type=F32)


def half_kernel(forcing_ref, start_ref, table_ref, out_ref):
    table = table_ref[...]
    start = start_ref[...]
    nothing = jnp.zeros_like(start)
    wide = jnp.concatenate(
        [
            jnp.concatenate([start, nothing], axis=1),
            jnp.concatenate([nothing, start], axis=1),
        ],
        axis=0,
    )
    packed = jnp.concatenate(
        [
            jnp.concatenate(
                [table[32 * slab : 32 * slab + 16], table[32 * slab + 16 : 32 * slab + 32]], axis=1
            )
            for slab in range(8)
        ],
        axis=0,
    )
    halved = dot(packed, wide, ((1,), (1,))).astype(BF16)
    for slab in range(8):
        out_ref[slab, pl.ds(MODES * PAIRS, 16), :] = halved[16 * slab : 16 * (slab + 1)]
    for pair in range(PAIRS):
        rows = forcing_ref[pl.ds(128 * pair, 128), :]
        halved = dot(table, rows, ((1,), (1,))).astype(BF16)
        for slab in range(8):
            out_ref[slab, pl.ds(MODES * pair, MODES), :] = halved[MODES * slab : MODES * (slab + 1)]


def source_kernel(
    turned_ref, table_ref, column_ref, row_ref, sources_ref, sums_ref, start_ref, local_ref
):
    gain, quad, mid, top = gains(slab_rates(column_ref, row_ref))
    for core in range(2):
        rows = MODES * PAIRS + (16 if core == 0 else 0)
        lhs = jnp.concatenate(
            [turned_ref[4 * core + (y + 2) % 4, pl.ds(0, rows), :] for y in range(4)], axis=1
        )
        spectra = dot(lhs, table_ref[...], ((1,), (0,)))
        for pair in range(PAIRS):
            for parity in range(2):
                part = spectra[
                    MODES * pair : MODES * (pair + 1), GRID * parity : GRID * (parity + 1)
                ]
                sources_ref[STEPS * core + 2 * pair + parity] = gain * part
        if core == 0:
            last = spectra[MODES * PAIRS :]
            start_ref[...] = jnp.concatenate([last[:, :GRID], last[:, GRID:]], axis=0)
    sums = []
    for point in range(CPOINTS):
        total = sources_ref[FINE_FACTOR * point]
        for step in range(1, FINE_FACTOR):
            total = gain * total + sources_ref[FINE_FACTOR * point + step]
        sums_ref[point] = total
        sums.append(total)
    begin = jnp.where(at_start(), start_ref[...], 0.0)
    leaving, _, _ = two_iterations((begin, None, begin, None), begin, sums, quad, mid, top)
    for index, array in enumerate(leaving):
        for side in range(2):
            local_ref[pl.ds(4 * side + index, MODES, stride=8), :] = array[
                :, 128 * side : 128 * (side + 1)
            ]


def scan_kernel(local_ref, column_ref, row_ref, state_ref):
    chip = (lax.axis_index("tm_0") + 2) % 4 * 16 + (lax.axis_index("tm_1") + 8) % 16
    column = column_ref[pl.ds(mode_slab() * MODES + chip // 2, 1), :]
    row = jnp.where(chip % 2 == 0, row_ref[:, :128], row_ref[:, 128:])
    _, quad, mid, top = gains(column + row)
    units = []
    for index in range(3):
        state = [None] * 4
        state[index] = jnp.ones_like(top)
        units.append(two_iterations(state, None, [None] * CPOINTS, quad, mid, top)[0])
    power = top
    for _ in range(1, TOPS):
        power = power * top
    relaxed = error = relaxed2 = error2 = jnp.zeros_like(top)
    for block in range(BLOCKS):
        place = PLANE_ORDER.index(block)
        for index, array in enumerate((relaxed, error, relaxed2, error2)):
            state_ref[pl.ds(4 * place + index, 1), :] = array
        local = [local_ref[pl.ds(4 * place + index, 1), :] for index in range(4)]
        error2 = power * error2 + (
            local[3] + units[0][3] * relaxed + units[1][3] * error + units[2][3] * relaxed2
        )
        relaxed2 = units[1][2] * error + (local[2] + units[0][2] * relaxed)
        error = power * error + (local[1] + units[0][1] * relaxed)
        relaxed = local[0]


def path_kernel(
    state_ref, sources_ref, sums_ref, start_ref, high_ref, low_ref, column_ref, row_ref, out_ref
):
    gain, quad, mid, top = gains(slab_rates(column_ref, row_ref))
    state = [
        jnp.concatenate(
            [state_ref[pl.ds(4 * side + index, MODES, stride=8), :] for side in range(2)], axis=1
        )
        for index in range(4)
    ]
    first = at_start()
    start = start_ref[...]
    begin = jnp.where(first, start, 0.0)
    state[0] = jnp.where(first, start, state[0])
    state[2] = jnp.where(first, start, state[2])
    sums = [sums_ref[point] for point in range(CPOINTS)]
    _, one, two = two_iterations(state, begin, sums, quad, mid, top)

    def square_sum(array):
        column = jnp.sum(array * array, axis=0, keepdims=True)
        return jnp.sum(column[:, :128] + column[:, 128:], axis=1, keepdims=True)

    lane = lax.broadcasted_iota(jnp.int32, (1, 128), 1)
    for core in range(2):
        lines = []
        for kind in range(3):
            for which in (one, two):
                line = jnp.zeros((1, 128), F32)
                for point in range(4):
                    total = square_sum(which[kind][4 * core + point])
                    line = jnp.where(lane % 4 == point, total, line)
                lines.append(line)
        lines = jnp.concatenate(lines + [jnp.zeros((10, 128), F32)], axis=0)
        upper = lines.astype(BF16).astype(F32)
        rest = lines - upper
        middle = rest.astype(BF16).astype(F32)
        group = lax.broadcasted_iota(jnp.int32, (16, 128), 1) // 4
        packed = jnp.where(
            group == 0,
            upper,
            jnp.where(group == 1, middle, jnp.where(group == 2, rest - middle, 0.0)),
        ).astype(BF16)
        for y in range(4):
            out_ref[4 * core + y, pl.ds(MODES * PAIRS, 16), :] = packed

    before = [state[2] + state[3]] + two[2][:-1]
    for core in range(2):
        rows = [[], []]
        for point in range(4 * core, 4 * core + 4):
            current = before[point]
            for step in range(FINE_FACTOR - 1):
                current = gain * current + sources_ref[FINE_FACTOR * point + step]
                rows[step % 2].append(current)
            rows[1].append(two[2][point])
        turned = []
        for parity in range(2):
            path = jnp.concatenate(rows[parity], axis=0)
            high = path.astype(BF16)
            low = (path - high.astype(F32)).astype(BF16)
            part = dot(high, high_ref[...], ((1,), (0,)))
            part += dot(high, low_ref[...], ((1,), (0,)))
            part += dot(low, high_ref[...], ((1,), (0,)))
            turned.append(part)
        left = lax.broadcasted_iota(jnp.int32, (MODES * PAIRS, 128), 1) < SLAB
        for group in range(2):
            even, odd = (part[:, 128 * group : 128 * (group + 1)] for part in turned)
            sides = (
                jnp.where(left, even, pltpu.roll(odd, SLAB, 1)),
                jnp.where(left, pltpu.roll(even, SLAB, 1), odd),
            )
            for side in range(2):
                place = 4 * core + (2 * group + side + 2) % 4
                out_ref[place, pl.ds(0, MODES * PAIRS), :] = sides[side].astype(BF16)


def heat_kernel(rows_ref, table_ref, heat_ref, history_ref, change_ref):
    table = table_ref[...]
    for pair in range(PAIRS):
        lhs = jnp.concatenate(
            [rows_ref[slab, pl.ds(MODES * pair, MODES), :] for slab in range(8)], axis=0
        )
        heat_ref[pl.ds(128 * pair, 128), :] = dot(lhs, table, ((0,), (0,)))
    total = jnp.zeros((16, 128), F32)
    for slab in range(8):
        total += rows_ref[slab, pl.ds(MODES * PAIRS, 16), :].astype(F32)
    total = total[:, 0:4] + total[:, 4:8] + total[:, 8:12]
    history_ref[...] = jnp.sqrt(total[0:2] / (GRID * GRID))
    change_ref[...] = jnp.sqrt(total[2:4] / total[4:6])


def call(kernel, outs, name):
    single = not isinstance(outs, (list, tuple))
    return pl.pallas_call(
        kernel,
        out_shape=outs if single else tuple(outs),
        compiler_params=pltpu.CompilerParams(vmem_limit_bytes=40 * 1024 * 1024),
        name=name,
    )


def per_device(forcing, starting_heat):
    half, low, inward = (jnp.asarray(c) for c in constants())
    mu = eigenvalues()
    columns = jnp.asarray(np.ascontiguousarray(np.broadcast_to(mu[:, None], (GRID, 128))))
    row = jnp.asarray(mu[None, :])
    shape = jax.ShapeDtypeStruct
    extent = MODES * PAIRS + 16
    ring = ("tm_2", "space")
    plane = ("tm_0", "tm_1")

    numbers = lax.optimization_barrier(jnp.arange(1, GRID + 1, dtype=jnp.int32))
    angles = numbers[:, None] * numbers[None, :] % (2 * (GRID + 1))
    angles = jnp.pi * angles.astype(F32) / (GRID + 1)
    table = (math.sqrt(2.0 / (GRID + 1)) * jnp.sin(angles)).astype(BF16)
    halved = call(half_kernel, shape((8, extent, 128), BF16), "half")(
        forcing.reshape(STEPS * SLAB, GRID), starting_heat, table
    )
    turned = exchange(halved, ring, RING_ORDER)
    sources, sums, start, local = call(
        source_kernel,
        [
            shape((2 * STEPS, MODES, GRID), F32),
            shape((CPOINTS, MODES, GRID), F32),
            shape((MODES, GRID), F32),
            shape((4 * BLOCKS, 128), F32),
        ],
        "source",
    )(turned, inward, columns, row)
    gathered = exchange(local.reshape(BLOCKS, 4, 128), plane, PLANE_ORDER)
    states = call(scan_kernel, shape((4 * BLOCKS, 128), F32), "scan")(
        gathered.reshape(4 * BLOCKS, 128), columns, row
    )
    state = exchange(states.reshape(BLOCKS, 4, 128), plane, PLANE_ORDER)
    rows = call(path_kernel, shape((8, extent, 128), BF16), "path")(
        state.reshape(4 * BLOCKS, 128), sources, sums, start, half, low, columns, row
    )
    returned = exchange(rows, ring, RING_ORDER)
    heat, history, change = call(
        heat_kernel,
        [shape((STEPS * SLAB, GRID), F32), shape((2, 4), F32), shape((2, 4), F32)],
        "heat",
    )(returned, half)
    return heat.reshape(STEPS, SLAB, GRID), history, change


def solution(mesh):
    torus = Mesh(
        mesh.devices.reshape(4, 16, 2, mesh.shape["space"]), ("tm_0", "tm_1", "tm_2", "space")
    )
    tm = ("tm_0", "tm_1", "tm_2")
    in_specs = (P(tm, "space", None), P("space", None))
    out_specs = (P(tm, "space", None), P(None, tm), P(None, tm))
    return jax.shard_map(
        per_device, mesh=torus, in_specs=in_specs, out_specs=out_specs, check_vma=False
    )
```

```python
import functools
import math

import jax
import jax.numpy as jnp
import numpy as np
from jax import lax
from jax.experimental import pallas as pl
from jax.experimental.pallas import tpu as pltpu
from jax.sharding import Mesh
from jax.sharding import PartitionSpec as P

FINE_FACTOR = 4
COARSE_FACTOR = 4
DURATION = 0.004
GRID = 256
NT = 2048
SLAB = 64
MODES = 32
STEPS = 16
PAIRS = STEPS // 2
TOPS = 2
CPOINTS = TOPS * COARSE_FACTOR
BLOCKS = 64
PLANE_ORDER = [((x + 2) % 4) * 16 + (z + 8) % 16 for x in range(4) for z in range(16)]
RING_ORDER = [core * 4 + (y + 2) % 4 for core in (1, 0) for y in range(4)]
F32, BF16 = jnp.float32, jnp.bfloat16


def sine_table():
    numbers = np.arange(1, GRID + 1)
    product = numbers[:, None] * numbers[None, :] % (2 * (GRID + 1))
    angles = np.float32(np.pi) * product.astype(np.float32) / np.float32(GRID + 1)
    sines = np.sin(angles.astype(np.float64)).astype(np.float32)
    return np.float32(math.sqrt(2.0 / (GRID + 1))) * sines


def eigenvalues():
    halves = np.sin(np.pi * np.arange(1, GRID + 1) / (2 * (GRID + 1)))
    return (4.0 * (GRID + 1) ** 2 * halves * halves).astype(np.float32)


def constants():
    full = sine_table()
    half = full.astype(jnp.bfloat16)
    low = (full - half.astype(np.float32)).astype(jnp.bfloat16)
    inward = np.zeros((4, 2, SLAB, 2, GRID), jnp.bfloat16)
    for k in range(2):
        inward[:, k, :, k, :] = half.reshape(4, SLAB, GRID)
    wide = 2 * GRID
    return half, low, inward.reshape(wide, wide)


def mul(a, b):
    return None if a is None or b is None else a * b


def add(a, b):
    return b if a is None else a if b is None else a + b


def sub(a, b):
    if b is None:
        return a
    return -b if a is None else a - b


def gains(rates):
    step = DURATION / NT
    gain = 1.0 / (1.0 + step * rates)
    mid = 1.0 / (1.0 + FINE_FACTOR * step * rates)
    top = 1.0 / (1.0 + FINE_FACTOR * COARSE_FACTOR * step * rates)
    square = gain * gain
    return gain, square * square, mid, top


def coarse_pass(entering, residual, mid, top):
    corrections = []
    for first in range(0, len(residual), COARSE_FACTOR):
        rows = residual[first : first + COARSE_FACTOR]
        running, inside = rows[0], entering
        for column in range(1, COARSE_FACTOR):
            inside = add(mul(mid, inside), rows[column - 1])
            corrections.append(inside)
            running = add(mul(mid, running), rows[column])
        entering = add(mul(top, entering), running)
        corrections.append(entering)
    return corrections, entering


def two_iterations(state, first_value, sums, quad, mid, top):
    relaxed_in, error_in, relaxed2_in, error2_in = state
    count = len(sums)
    relaxed = [add(mul(quad, first_value), sums[0])] + list(sums[1:])
    residual = [mul(quad, sub(relaxed_in, first_value))]
    residual += [mul(quad, relaxed[c - 1]) for c in range(1, count)]
    fix, error_out = coarse_pass(error_in, residual, mid, top)
    values = [add(r, p) for r, p in zip(relaxed, fix)]
    before = [add(relaxed_in, error_in)] + values[:-1]
    relaxed2 = [add(mul(quad, v), s) for v, s in zip(before, sums)]
    residual2 = [
        mul(quad, sub(r, v)) for r, v in zip([relaxed2_in] + relaxed2[:-1], before)
    ]
    fix2, error2_out = coarse_pass(error2_in, residual2, mid, top)
    values2 = [add(r, p) for r, p in zip(relaxed2, fix2)]
    leaving = (relaxed[-1], error_out, relaxed2[-1], error2_out)
    return leaving, (residual, fix, values), (residual2, fix2, values2)


def at_start():
    return jnp.logical_and(lax.axis_index("tm_0") == 0, lax.axis_index("tm_1") == 0)


def mode_slab():
    return (1 - lax.axis_index("tm_2")) * 4 + (lax.axis_index("space") + 2) % 4


def exchange(array, axes, order):
    return lax.all_to_all(array, axes, 0, 0, axis_index_groups=[order], tiled=True)


def slab_rates(column_ref, row_ref):
    first = pl.multiple_of(mode_slab() * MODES, MODES)
    columns = column_ref[pl.ds(first, MODES), :]
    return jnp.concatenate([columns, columns], axis=1) + row_ref[...]


def dot(a, b, dims):
    return lax.dot_general(a, b, (dims, ((), ())), preferred_element_type=F32)


def half_kernel(forcing_ref, start_ref, table_ref, out_ref):
    table = table_ref[...]
    start = start_ref[...]
    nothing = jnp.zeros_like(start)
    wide = jnp.concatenate(
        [
            jnp.concatenate([start, nothing], axis=1),
            jnp.concatenate([nothing, start], axis=1),
        ],
        axis=0,
    )
    packed = jnp.concatenate(
        [
            jnp.concatenate(
                [table[32 * slab : 32 * slab + 16], table[32 * slab + 16 : 32 * slab + 32]], axis=1
            )
            for slab in range(8)
        ],
        axis=0,
    )
    halved = dot(packed, wide, ((1,), (1,))).astype(BF16)
    for slab in range(8):
        out_ref[slab, pl.ds(MODES * PAIRS, 16), :] = halved[16 * slab : 16 * (slab + 1)]
    for pair in range(PAIRS):
        rows = forcing_ref[pl.ds(128 * pair, 128), :]
        halved = dot(table, rows, ((1,), (1,))).astype(BF16)
        for slab in range(8):
            out_ref[slab, pl.ds(MODES * pair, MODES), :] = halved[MODES * slab : MODES * (slab + 1)]


def source_kernel(
    turned_ref, table_ref, column_ref, row_ref, sources_ref, sums_ref, start_ref, local_ref
):
    gain, quad, mid, top = gains(slab_rates(column_ref, row_ref))
    for core in range(2):
        rows = MODES * PAIRS + (16 if core == 0 else 0)
        lhs = jnp.concatenate(
            [turned_ref[4 * (1 - core) + (y + 2) % 4, pl.ds(0, rows), :] for y in range(4)], axis=1
        )
        spectra = dot(lhs, table_ref[...], ((1,), (0,)))
        for pair in range(PAIRS):
            for parity in range(2):
                part = spectra[
                    MODES * pair : MODES * (pair + 1), GRID * parity : GRID * (parity + 1)
                ]
                sources_ref[STEPS * core + 2 * pair + parity] = gain * part
        if core == 0:
            last = spectra[MODES * PAIRS :]
            start_ref[...] = jnp.concatenate([last[:, :GRID], last[:, GRID:]], axis=0)
    sums = []
    for point in range(CPOINTS):
        total = sources_ref[FINE_FACTOR * point]
        for step in range(1, FINE_FACTOR):
            total = gain * total + sources_ref[FINE_FACTOR * point + step]
        sums_ref[point] = total
        sums.append(total)
    begin = jnp.where(at_start(), start_ref[...], 0.0)
    leaving, _, _ = two_iterations((begin, None, begin, None), begin, sums, quad, mid, top)
    for index, array in enumerate(leaving):
        for side in range(2):
            local_ref[pl.ds(4 * side + index, MODES, stride=8), :] = array[
                :, 128 * side : 128 * (side + 1)
            ]


def scan_kernel(local_ref, column_ref, row_ref, state_ref):
    chip = (lax.axis_index("tm_0") + 2) % 4 * 16 + (lax.axis_index("tm_1") + 8) % 16
    column = column_ref[pl.ds(mode_slab() * MODES + chip // 2, 1), :]
    row = jnp.where(chip % 2 == 0, row_ref[:, :128], row_ref[:, 128:])
    _, quad, mid, top = gains(column + row)
    units = []
    for index in range(3):
        state = [None] * 4
        state[index] = jnp.ones_like(top)
        units.append(two_iterations(state, None, [None] * CPOINTS, quad, mid, top)[0])
    power = top
    for _ in range(1, TOPS):
        power = power * top
    relaxed = error = relaxed2 = error2 = jnp.zeros_like(top)
    for block in range(BLOCKS):
        place = PLANE_ORDER.index(block)
        for index, array in enumerate((relaxed, error, relaxed2, error2)):
            state_ref[pl.ds(4 * place + index, 1), :] = array
        local = [local_ref[pl.ds(4 * place + index, 1), :] for index in range(4)]
        error2 = power * error2 + (
            local[3] + units[0][3] * relaxed + units[1][3] * error + units[2][3] * relaxed2
        )
        relaxed2 = units[1][2] * error + (local[2] + units[0][2] * relaxed)
        error = power * error + (local[1] + units[0][1] * relaxed)
        relaxed = local[0]


def path_kernel(
    state_ref, sources_ref, sums_ref, start_ref, high_ref, low_ref, column_ref, row_ref, out_ref
):
    gain, quad, mid, top = gains(slab_rates(column_ref, row_ref))
    state = [
        jnp.concatenate(
            [state_ref[pl.ds(4 * side + index, MODES, stride=8), :] for side in range(2)], axis=1
        )
        for index in range(4)
    ]
    first = at_start()
    start = start_ref[...]
    begin = jnp.where(first, start, 0.0)
    state[0] = jnp.where(first, start, state[0])
    state[2] = jnp.where(first, start, state[2])
    sums = [sums_ref[point] for point in range(CPOINTS)]
    _, one, two = two_iterations(state, begin, sums, quad, mid, top)

    def square_sum(array):
        column = jnp.sum(array * array, axis=0, keepdims=True)
        return jnp.sum(column[:, :128] + column[:, 128:], axis=1, keepdims=True)

    lane = lax.broadcasted_iota(jnp.int32, (1, 128), 1)
    for core in range(2):
        lines = []
        for kind in range(3):
            for which in (one, two):
                line = jnp.zeros((1, 128), F32)
                for point in range(4):
                    total = square_sum(which[kind][4 * core + point])
                    line = jnp.where(lane % 4 == point, total, line)
                lines.append(line)
        lines = jnp.concatenate(lines + [jnp.zeros((10, 128), F32)], axis=0)
        upper = lines.astype(BF16).astype(F32)
        rest = lines - upper
        middle = rest.astype(BF16).astype(F32)
        group = lax.broadcasted_iota(jnp.int32, (16, 128), 1) // 4
        packed = jnp.where(
            group == 0,
            upper,
            jnp.where(group == 1, middle, jnp.where(group == 2, rest - middle, 0.0)),
        ).astype(BF16)
        for y in range(4):
            out_ref[4 * (1 - core) + y, pl.ds(MODES * PAIRS, 16), :] = packed

    before = [state[2] + state[3]] + two[2][:-1]
    for core in range(2):
        rows = [[], []]
        for point in range(4 * core, 4 * core + 4):
            current = before[point]
            for step in range(FINE_FACTOR - 1):
                current = gain * current + sources_ref[FINE_FACTOR * point + step]
                rows[step % 2].append(current)
            rows[1].append(two[2][point])
        turned = []
        for parity in range(2):
            path = jnp.concatenate(rows[parity], axis=0)
            high = path.astype(BF16)
            low = (path - high.astype(F32)).astype(BF16)
            part = dot(high, high_ref[...], ((1,), (0,)))
            part += dot(high, low_ref[...], ((1,), (0,)))
            part += dot(low, high_ref[...], ((1,), (0,)))
            turned.append(part)
        left = lax.broadcasted_iota(jnp.int32, (MODES * PAIRS, 128), 1) < SLAB
        for group in range(2):
            even, odd = (part[:, 128 * group : 128 * (group + 1)] for part in turned)
            sides = (
                jnp.where(left, even, pltpu.roll(odd, SLAB, 1)),
                jnp.where(left, pltpu.roll(even, SLAB, 1), odd),
            )
            for side in range(2):
                place = 4 * (1 - core) + (2 * group + side + 2) % 4
                out_ref[place, pl.ds(0, MODES * PAIRS), :] = sides[side].astype(BF16)


def heat_kernel(rows_ref, table_ref, heat_ref, history_ref, change_ref):
    table = table_ref[...]
    for pair in range(PAIRS):
        lhs = jnp.concatenate(
            [rows_ref[slab, pl.ds(MODES * pair, MODES), :] for slab in range(8)], axis=0
        )
        heat_ref[pl.ds(128 * pair, 128), :] = dot(lhs, table, ((0,), (0,)))
    total = jnp.zeros((16, 128), F32)
    for slab in range(8):
        total += rows_ref[slab, pl.ds(MODES * PAIRS, 16), :].astype(F32)
    total = total[:, 0:4] + total[:, 4:8] + total[:, 8:12]
    history_ref[...] = jnp.sqrt(total[0:2] / (GRID * GRID))
    change_ref[...] = jnp.sqrt(total[2:4] / total[4:6])


def call(kernel, outs, name):
    single = not isinstance(outs, (list, tuple))
    return pl.pallas_call(
        kernel,
        out_shape=outs if single else tuple(outs),
        compiler_params=pltpu.CompilerParams(vmem_limit_bytes=40 * 1024 * 1024),
        name=name,
    )


def per_device(forcing, starting_heat):
    half, low, inward = (jnp.asarray(c) for c in constants())
    mu = eigenvalues()
    columns = jnp.asarray(np.ascontiguousarray(np.broadcast_to(mu[:, None], (GRID, 128))))
    row = jnp.asarray(mu[None, :])
    shape = jax.ShapeDtypeStruct
    extent = MODES * PAIRS + 16
    ring = ("tm_2", "space")
    plane = ("tm_0", "tm_1")

    numbers = lax.optimization_barrier(jnp.arange(1, GRID + 1, dtype=jnp.int32))
    angles = numbers[:, None] * numbers[None, :] % (2 * (GRID + 1))
    angles = jnp.pi * angles.astype(F32) / (GRID + 1)
    table = (math.sqrt(2.0 / (GRID + 1)) * jnp.sin(angles)).astype(BF16)
    halved = call(half_kernel, shape((8, extent, 128), BF16), "half")(
        forcing.reshape(STEPS * SLAB, GRID), starting_heat, table
    )
    turned = exchange(halved, ring, RING_ORDER)
    sources, sums, start, local = call(
        source_kernel,
        [
            shape((2 * STEPS, MODES, GRID), F32),
            shape((CPOINTS, MODES, GRID), F32),
            shape((MODES, GRID), F32),
            shape((4 * BLOCKS, 128), F32),
        ],
        "source",
    )(turned, inward, columns, row)
    gathered = exchange(local.reshape(BLOCKS, 4, 128), plane, PLANE_ORDER)
    states = call(scan_kernel, shape((4 * BLOCKS, 128), F32), "scan")(
        gathered.reshape(4 * BLOCKS, 128), columns, row
    )
    state = exchange(states.reshape(BLOCKS, 4, 128), plane, PLANE_ORDER)
    rows = call(path_kernel, shape((8, extent, 128), BF16), "path")(
        state.reshape(4 * BLOCKS, 128), sources, sums, start, half, low, columns, row
    )
    returned = exchange(rows, ring, RING_ORDER)
    heat, history, change = call(
        heat_kernel,
        [shape((STEPS * SLAB, GRID), F32), shape((2, 4), F32), shape((2, 4), F32)],
        "heat",
    )(returned, half)
    return heat.reshape(STEPS, SLAB, GRID), history, change


def solution(mesh):
    torus = Mesh(
        mesh.devices.reshape(4, 16, 2, mesh.shape["space"]), ("tm_0", "tm_1", "tm_2", "space")
    )
    tm = ("tm_0", "tm_1", "tm_2")
    in_specs = (P(tm, "space", None), P("space", None))
    out_specs = (P(tm, "space", None), P(None, tm), P(None, tm))
    return jax.shard_map(
        per_device, mesh=torus, in_specs=in_specs, out_specs=out_specs, check_vma=False
    )
```
